256 devices in a mesh: ka: 64 (over x, z_hi, y), slab: 4 (over z_lo, core).
Axes of the slice: x: 4, y: 4, z: 8 (z_hi: 4, z_lo: 2; z = z_hi * 2 + z_lo), core: 2. Of those that a mesh axis runs over, the one named last changes fastest.
Arguments:
- val_wave: float32 [2, 64, 2, 12, 16, 128], P(None, 'ka', None, 'slab'), may hold values from -6 to 6
- cond_wave: float32 [2, 64, 8, 12, 16, 128], P(None, 'ka', None, 'slab'), may hold values from -6 to 6
- val_energy: float32 [64, 2], P('ka'), may hold values from -2 to -0.5
- cond_energy: float32 [64, 8], P('ka'), may hold values from 0.5 to 3
- frequency: float32 [4], replicated, may hold values from 0.2 to 4
- kpoint_map: int32 [64], replicated, may hold values from 0 to 63, as said below
- umklapp: int32 [3, 64], replicated, may hold values from 0 to 1, as said below
- gvector_index: int32 [6144], replicated, may hold values from 0 to 24575, as said below
Outputs:
- polarizability: float32 [4, 2, 6144, 6144], P(None, None, 'ka', 'slab')
The draws below stay inside these ranges and needn't reach their ends.
Inputs may be any that keep to these rules, and one draw needn't show every extreme that they name: With s the integer for which s * s * s = 64 and k = s * s * i + s * j + l, kpoint_map[k] is the index of (i + q0, j + q1, l + q2) taken modulo s in each coordinate, for one vector q whose components lie in 0 to s - 1, not all zero. umklapp[d, k] is 1 where coordinate d of k plus component d of q reaches s, else 0. `gvector_index`: entries are distinct.
All inputs are finite; a program needn't handle non-finite values.
Results may differ from the reference program's by a relative error of at most 0.0038.
Values may be sent and summed in bfloat16 or wider, within the bound.
A program may use at most 128 MiB of HBM per device.

```python
import math
import jax
import jax.numpy as jnp
from jax import lax

NV = 2
NC = 8
GX = 12
GY = 16
GZ = 128
NG = 6144
NW = 4
NK = 64
N_KA = 64


def grid_parts(key):
    grid_side = max((candidate for candidate in range(1, 9) if candidate ** 3 <= N_KA))
    flat_shift = jax.random.randint(jax.random.fold_in(key, 29), (), 1, grid_side ** 3)
    shift = [flat_shift // grid_side ** (2 - grid_dim) % grid_side for grid_dim in range(3)]
    index = jnp.arange(N_KA, dtype=jnp.int32)
    moved = [index // grid_side ** (2 - grid_dim) % grid_side + shift[grid_dim] for grid_dim in range(3)]
    mapped = sum((moved[grid_dim] % grid_side * grid_side ** (2 - grid_dim) for grid_dim in range(3)))
    folded = jnp.stack([(moved[grid_dim] >= grid_side).astype(jnp.int32) for grid_dim in range(3)])
    return (mapped.astype(jnp.int32), folded)


def draw_kpoint_map(key, part):
    return grid_parts(key)[0]


def draw_umklapp(key, part):
    return grid_parts(key)[1]


def draw_gvector_index(key, part):
    return jax.random.permutation(key, GX * GY * GZ)[:NG].astype(jnp.int32)


def block_levels(stream_key, shape, split, smallest, high):
    gain, own = 1.0, jax.random.fold_in(stream_key, 6)
    for position, shards_of in split:
        heights = jnp.exp(jax.random.uniform(jax.random.fold_in(own, position), (shards_of,), jnp.float32, smallest / len(split), high / len(split)))
        gain = gain * jnp.repeat(heights, shape[position] // shards_of).reshape([-1 if axis == position else 1 for axis in range(len(shape))])
    return gain


def gaussian(own_key, shape, spread, limit, cuts=(), held_as=jnp.bfloat16):
    level = block_levels(own_key, shape, cuts, -0.22, 0.18) if cuts else 1.0
    drawn = jax.random.normal(own_key, shape, jnp.float32) * spread * level
    return jnp.minimum(jnp.maximum(drawn, -limit), limit).astype(held_as)


def setup_inputs(seed: int = 0) -> dict:
    streams_of = jax.random.split(jax.random.key(seed), 9)
    return {
        "val_wave": gaussian(streams_of[0], (2, NK, NV, GX, GY, GZ), 1.0, 6.0, ((1, 64), (3, 4)), jnp.float32),
        "cond_wave": gaussian(streams_of[1], (2, NK, NC, GX, GY, GZ), 1.0, 6.0, ((1, 64), (3, 4)), jnp.float32),
        "val_energy": jnp.clip(-2.0 + 1.5 * jax.random.uniform(streams_of[2], (NK, NV), jnp.float32) ** block_levels(streams_of[2], (NK, NV), ((0, 64),), -0.2, 0.2), -2.0, -0.5),
        "cond_energy": jnp.clip(0.5 + 2.5 * jax.random.uniform(streams_of[3], (NK, NC), jnp.float32) ** block_levels(streams_of[3], (NK, NC), ((0, 64),), -0.2, 0.2), 0.5, 3.0),
        "frequency": jnp.clip(jnp.exp(jax.random.uniform(streams_of[4], (NW,), jnp.float32, math.log(0.2), math.log(4.0))), 0.2, 4.0),
        "kpoint_map": draw_kpoint_map(jax.random.fold_in(streams_of[8], 71), 0),
        "umklapp": draw_umklapp(jax.random.fold_in(streams_of[8], 71), 0),
        "gvector_index": draw_gvector_index(jax.random.fold_in(streams_of[8], 71), 0),
    }


two_pi = 2.0 * math.pi

def phase_angle(shift_vec, xpos, ypos, zpos):
    first_part = (shift_vec[0] * xpos % GX).astype(jnp.float32)[:, None, None] / GX
    second_part = (shift_vec[1] * ypos % GY).astype(jnp.float32)[None, :, None] / GY
    third_part = (shift_vec[2] * zpos % GZ).astype(jnp.float32)[None, None, :] / GZ
    return two_pi * (first_part + second_part + third_part)

def reference(val_wave, cond_wave, val_energy, cond_energy, frequency, kpoint_map, umklapp, gvector_index):
    pairs = NV * NC
    points = GX * GY * GZ
    kcount = val_wave.shape[1]
    xpos = jnp.arange(GX, dtype=jnp.int32)
    ypos = jnp.arange(GY, dtype=jnp.int32)
    zpos = jnp.arange(GZ, dtype=jnp.int32)
    norm = 1.0 / (2.0 * math.sqrt(points))

    def one_point(kpoint):
        valence = val_wave[:, kpoint]
        conduct = cond_wave[:, kpoint_map[kpoint]]
        angle = phase_angle(umklapp[:, kpoint], xpos, ypos, zpos)
        rotor = jnp.cos(angle) + 1j * jnp.sin(angle)
        cwave = (conduct[0] + 1j * conduct[1]) * rotor
        vwave = valence[0] + 1j * valence[1]
        density = (jnp.conj(vwave)[:, None] * cwave[None]).reshape(pairs, GX, GY, GZ)
        spectrum = jnp.fft.fftn(density, axes=(1, 2, 3)).reshape(pairs, points)[:, gvector_index] * norm
        return jnp.stack([jnp.real(spectrum), jnp.imag(spectrum)]).astype(jnp.float32)
    pair = lax.map(one_point, jnp.arange(kcount, dtype=jnp.int32))
    gap = (val_energy[:, :, None] - cond_energy[kpoint_map][:, None, :]).reshape(kcount, pairs)
    weight = 2.0 * gap[:, None, :] / (gap[:, None, :] ** 2 + frequency[None, :, None] ** 2) / kcount
    pair_low = lax.optimization_barrier(pair.astype(jnp.bfloat16)).astype(jnp.float32)
    right = jnp.concatenate([pair_low[:, 0].reshape(kcount * pairs, NG), pair_low[:, 1].reshape(kcount * pairs, NG)], 0)
    dims = (((0,), (0,)), ((), ()))

    def one_freq(weight_col):
        scaled = lax.optimization_barrier((pair * weight_col[:, None, :, None]).astype(jnp.bfloat16)).astype(jnp.float32)
        real_part = scaled[:, 0].reshape(kcount * pairs, NG)
        imag_part = scaled[:, 1].reshape(kcount * pairs, NG)
        left_re = jnp.concatenate([real_part, imag_part], 0)
        left_im = jnp.concatenate([imag_part, -real_part], 0)
        out_re = lax.dot_general(left_re, right, dims, preferred_element_type=jnp.float32)
        out_im = lax.dot_general(left_im, right, dims, preferred_element_type=jnp.float32)
        return jnp.stack([out_re, out_im])
    return lax.map(one_freq, jnp.transpose(weight, (1, 0, 2)))
```

```python
import math

import jax
import jax.numpy as jnp
import numpy as np
from jax import lax
from jax.experimental import pallas as pl
from jax.experimental.pallas import tpu as pltpu
from jax.sharding import PartitionSpec as P

two_pi = 2.0 * math.pi
HIGH = lax.Precision.HIGHEST


def cut_along(shard, dim, count):
    dims = shard.shape
    parts = shard.reshape(*dims[:dim], count, dims[dim] // count, *dims[dim + 1 :])
    return jnp.moveaxis(parts, dim, 0)


def summed_on_arrival(shard, axis, dim):
    parts = cut_along(shard, dim, lax.axis_size(axis))
    arrived = lax.all_to_all(parts, axis, split_axis=0, concat_axis=0, tiled=True)
    return arrived.sum(axis=0)


def laid_out(parts, dim):
    dims = list(parts.shape[1:])
    dims[dim] *= parts.shape[0]
    return jnp.moveaxis(parts, 0, dim).reshape(dims)


def copy_for_each(shard, axis):
    copies = jnp.broadcast_to(shard, (lax.axis_size(axis), *shard.shape))
    return lax.all_to_all(copies, axis, split_axis=0, concat_axis=0, tiled=True)


def gather_directly(shard, axis, dim):
    return laid_out(copy_for_each(shard, axis), dim)


def y_table():
    y = np.arange(16)
    ang = 2*np.pi*(np.outer(y, y) % 16)/16
    eye = np.eye(8)
    c = np.einsum("ky,cd->kcdy", np.cos(ang), eye).reshape(128, 128)
    s = np.einsum("ky,cd->kcdy", np.sin(ang), eye).reshape(128, 128)
    return np.block([[c, s], [-s, c]]).astype(np.float32)

def z_table():
    z = np.arange(128)
    ang = 2*np.pi*(np.outer(z, z) % 128)/128
    c, s = np.cos(ang), np.sin(ang)
    return np.block([[c, -s], [s, c]]).astype(np.float32)

TILE = 256

def pair_kernel(val, cond, gy, gz, xc, xs, ly, wz, out, spec):
    planes = val.shape[2]
    for v in range(2):
        for x in range(planes):
            vr, vi = val[0, v, x][None], val[1, v, x][None]
            cr, ci = cond[0, :, x], cond[1, :, x]
            re = (vr * cr + vi * ci).reshape(128, 128)
            im = (vr * ci - vi * cr).reshape(128, 128)
            t = jnp.dot(ly[...], jnp.concatenate([re, im], 0), precision=HIGH, preferred_element_type=jnp.float32)
            f = jnp.dot(jnp.concatenate([t[:128], t[128:]], 1), wz[...], precision=HIGH, preferred_element_type=jnp.float32)
            both = jnp.concatenate([f[:, :128].reshape(16, 8, 128), f[:, 128:].reshape(16, 8, 128)], 1)
            hi = both.astype(jnp.bfloat16)
            spec[:, v*planes+x, :, :128] = hi
            spec[:, v*planes+x, :, 128:] = (both - hi.astype(jnp.float32)).astype(jnp.bfloat16)
    groups = 2*planes
    table = spec[...].reshape(16*groups*16, 256)

    def step(i, _):
        cols = pl.ds(pl.multiple_of(i*TILE, TILE), TILE)
        hot = (lax.broadcasted_iota(jnp.int32, (128, TILE), 0) == gz[:, cols]).astype(jnp.float32).astype(jnp.bfloat16)
        picked = jnp.dot(spec[...].reshape(16*groups*16, 256), jnp.concatenate([hot, hot], 0), preferred_element_type=jnp.float32)
        which = jnp.broadcast_to(gy[:, cols], (16*groups, TILE))
        acc = picked[:16*groups]
        for ky in range(1, 16):
            acc = jnp.where(which == ky, picked[ky*16*groups:(ky+1)*16*groups], acc)
        for v in range(2):
            re, im = 0.0, 0.0
            for x in range(planes):
                at = (v*planes+x)*16
                c, s = xc[x:x+1, cols], xs[x:x+1, cols]
                sre, sim = acc[at:at+8], acc[at+8:at+16]
                re = re + (sre*c + sim*s)
                im = im + (sim*c - sre*s)
            out[0, v*8:v*8+8, cols] = re
            out[1, v*8:v*8+8, cols] = im
        return 0
    lax.fori_loop(0, out.shape[2]//TILE, step, 0)

def pair_call(val, cond, gy, gz, xc, xs):
    total = gy.shape[1]
    vm = pl.BlockSpec(memory_space=pltpu.VMEM)
    return pl.pallas_call(
        pair_kernel, out_shape=jax.ShapeDtypeStruct((2, 16, total), jnp.float32),
        in_specs=[vm]*8, out_specs=vm,
        scratch_shapes=[pltpu.VMEM((16, 2*val.shape[2], 16, 256), jnp.bfloat16)],
        cost_estimate=pl.CostEstimate(flops=10_000_000_000, bytes_accessed=4_000_000, transcendentals=0),
        name="pairs",
    )(val, cond, gy, gz, xc, xs, jnp.asarray(y_table()), jnp.asarray(z_table()))

def shifted_target(index, shift, side):
    target = 0
    for stride in (side * side, side, 1):
        target += (index // stride + shift // stride) % side * stride
    return target


def route(payload, shift, side):
    count = side**3

    def along(offset):
        pairs = [(i, shifted_target(i, offset, side)) for i in range(count)]
        return lambda block: lax.ppermute(block, "ka", pairs)

    middle = shift // side % side
    outer = shift // (side * side) * side + shift % side
    ends = [i // side * side * side + i % side for i in range(1, side * side)]
    payload = lax.switch(middle, [lambda block: block] + [along(i * side) for i in range(1, side)], payload)
    return lax.switch(outer, [lambda block: block] + [along(i) for i in ends], payload)


def per_device(
    val_wave, cond_wave, val_energy, cond_energy, frequency, kpoint_map, umklapp, gvector_index
):
    slab_count = lax.axis_size("slab")
    kpoint_count = lax.axis_size("ka")
    here = lax.axis_index("ka")
    slab_here = lax.axis_index("slab")
    side = max((candidate for candidate in range(1, 9) if candidate**3 <= kpoint_count))
    shift = kpoint_map[0]
    planes, extent_y, extent_z = val_wave.shape[3:]
    fields = val_wave.shape[0] * val_wave.shape[2] * planes
    levels = jnp.pad(val_energy, ((0, extent_y - 1), (0, extent_z - val_energy.shape[1])))
    packed = jnp.concatenate([val_wave.reshape(fields, extent_y, extent_z), levels[None]], 0)
    packed = route(packed, shift, side)
    valence = packed[:fields].reshape(2, -1, planes, extent_y, extent_z)
    val_energy = packed[fields, :1, : val_energy.shape[1]]
    strides = [side * side, side, 1]
    wrapped = [(here // d % side < shift // d % side).astype(jnp.int32) for d in strides]
    extent_x = planes * slab_count
    gz_idx = (gvector_index % extent_z - wrapped[2]) % extent_z
    gy_idx = (gvector_index // extent_z % extent_y - wrapped[1]) % extent_y
    gx_idx = gvector_index // (extent_y * extent_z) - wrapped[0] + extent_x
    xpos = slab_here * planes + jnp.arange(planes, dtype=jnp.int32)
    xangle = two_pi * (xpos[:, None] * gx_idx[None, :] % extent_x).astype(jnp.float32) / extent_x
    norm = 1.0 / (2.0 * math.sqrt(extent_x * extent_y * extent_z))
    xcos = jnp.cos(xangle) * norm
    xsin = jnp.sin(xangle) * norm
    partial_value = pair_call(valence, cond_wave[:, 0], gy_idx[None], gz_idx[None], xcos, xsin)
    pairs = partial_value.shape[1]
    gap = (val_energy[0][:, None] - cond_energy[0][None, :]).reshape(pairs)
    weight = 2.0 * gap[None, :] / (gap[None, :] ** 2 + frequency[:, None] ** 2) / kpoint_count
    freq_count = frequency.shape[0]
    total_g = gvector_index.shape[0]
    block_g = total_g // slab_count
    row_g = total_g // kpoint_count
    block = summed_on_arrival(partial_value, "slab", 2)
    column_side = block.astype(jnp.bfloat16)
    pair_full = gather_directly(block, "slab", 2)
    moved = lax.all_to_all(pair_full[:, None], "ka", split_axis=3, concat_axis=1, tiled=True)
    weight_all = gather_directly(weight[None], "ka", 0)
    routed = (
        moved[:, :, :, None, :] * jnp.transpose(weight_all, (0, 2, 1))[None, :, :, :, None]
    ).astype(jnp.bfloat16)
    columns = lax.all_gather(column_side[:, None], "ka", axis=1, tiled=True)
    flat_rows = kpoint_count * pairs
    real_rows = routed[0].reshape(flat_rows, freq_count, row_g)
    imag_rows = routed[1].reshape(flat_rows, freq_count, row_g)
    left = jnp.stack(
        [jnp.concatenate([real_rows, imag_rows], 0), jnp.concatenate([imag_rows, -real_rows], 0)],
        axis=2,
    )
    left = left.reshape(2 * flat_rows, freq_count * 2 * row_g)
    right = columns.reshape(2 * flat_rows, block_g)
    product = lax.dot_general(
        left, right, (((0,), (0,)), ((), ())), preferred_element_type=jnp.float32
    )
    return product.reshape(freq_count, 2, row_g, block_g)


def solution(mesh):
    return jax.shard_map(
        per_device,
        mesh=mesh,
        in_specs=(
            P(None, "ka", None, "slab", None, None),
            P(None, "ka", None, "slab", None, None),
            P("ka", None),
            P("ka", None),
            P(),
            P(),
            P(),
            P(),
        ),
        out_specs=P(None, None, "ka", "slab"),
        check_vma=False,
    )
```

```python
import functools
import math

import jax
import jax.numpy as jnp
import numpy as np
from jax import lax
from jax.experimental import pallas as pl
from jax.experimental.pallas import tpu as pltpu
from jax.sharding import PartitionSpec as P

HIGH = lax.Precision.HIGHEST
MESH = pl.DeviceIdType.MESH
f32, bf16 = jnp.float32, jnp.bfloat16
TILE = 256


def y_table(bands, extent):
    index = np.arange(extent)
    angle = 2 * np.pi * (np.outer(index, index) % extent) / extent
    eye = np.eye(bands)
    size = bands * extent
    cos = np.einsum("ky,cd->kcdy", np.cos(angle), eye).reshape(size, size)
    sin = np.einsum("ky,cd->kcdy", np.sin(angle), eye).reshape(size, size)
    return np.block([[cos, sin], [-sin, cos]]).astype(np.float32)


def z_table(extent):
    index = np.arange(extent)
    angle = 2 * np.pi * (np.outer(index, index) % extent) / extent
    cos, sin = np.cos(angle), np.sin(angle)
    return np.block([[cos, -sin], [sin, cos]]).astype(np.float32)


def x_table(extent, norm):
    index = np.arange(extent)
    angle = 2 * np.pi * (np.outer(index, index) % extent) / extent
    return (np.concatenate([np.cos(angle), np.sin(angle)], 1) * norm).astype(np.float32)


def pair_kernel(count, scalars, xtab, freq, cond_e, packed, cond, gvec, ytab, ztab, out, wout, spec):
    bands, planes, ny, nz = cond.shape[1:]
    nv = 2
    nx = xtab.shape[0]
    rows = bands * ny
    groups = nv * planes
    fields = nv * 2 * planes
    for v in range(nv):
        for x in range(planes):
            vr = packed[v * planes + x][None]
            vi = packed[(nv + v) * planes + x][None]
            cr, ci = cond[0, :, x], cond[1, :, x]
            re = (vr * cr + vi * ci).reshape(rows, nz)
            im = (vr * ci - vi * cr).reshape(rows, nz)
            t = jnp.dot(ytab[...], jnp.concatenate([re, im], 0), precision=HIGH, preferred_element_type=f32)
            t = jnp.concatenate([t[:rows], t[rows:]], 1)
            f = jnp.dot(t, ztab[...], precision=HIGH, preferred_element_type=f32)
            parts = [f[:, :nz].reshape(ny, bands, nz), f[:, nz:].reshape(ny, bands, nz)]
            both = jnp.concatenate(parts, 1)
            high = both.astype(bf16)
            spec[:, v * planes + x, :, :nz] = high
            spec[:, v * planes + x, :, nz:] = (both - high.astype(f32)).astype(bf16)

    lane = lax.broadcasted_iota(jnp.int32, (2 * bands, 128), 1)
    row = lax.broadcasted_iota(jnp.int32, (2 * bands, 128), 0)
    level = jnp.zeros((2 * bands, 128), f32)
    for c in range(bands):
        level = jnp.where((row == c) | (row == bands + c), cond_e[0, c], level)
    omega = jnp.zeros((2 * bands, 128), f32)
    for w in range(freq.shape[0]):
        omega = jnp.where((lane >= 3 * w) & (lane < 3 * w + 3), freq[w], omega)
    piece = lane - lane // 3 * 3
    for v in range(nv):
        gap = packed[fields, 0:1, v : v + 1] - level
        weight = 2.0 * gap / (gap * gap + omega * omega) / count
        high = weight.astype(bf16).astype(f32)
        mid = (weight - high).astype(bf16).astype(f32)
        low = weight - high - mid
        value = jnp.where(piece == 0, high, jnp.where(piece == 1, mid, low))
        wout[v] = jnp.where(lane < 3 * freq.shape[0], value, 0.0).astype(bf16)

    per_block = out.shape[4] // TILE

    def step(i, _):
        g = gvec[:, pl.ds(pl.multiple_of(i * TILE, TILE), TILE)]
        gz = (g % nz - scalars[2] + nz) % nz
        gy = (g // nz % ny - scalars[1] + ny) % ny
        gx = g // (nz * ny) - scalars[0]
        gx = jnp.where(gx < 0, gx + nx, gx)
        hot = (lax.broadcasted_iota(jnp.int32, (nz, TILE), 0) == gz).astype(f32).astype(bf16)
        hot = jnp.concatenate([hot, hot], 0)
        table = spec[...].reshape(ny * groups * 2 * bands, 2 * nz)
        picked = jnp.dot(table, hot, preferred_element_type=f32)
        height = groups * 2 * bands
        which = jnp.broadcast_to(gy, (height, TILE))
        acc = picked[:height]
        for ky in range(1, ny):
            acc = jnp.where(which == ky, picked[ky * height : (ky + 1) * height], acc)
        cosines = [jnp.zeros((1, TILE), f32) for _ in range(planes)]
        sines = list(cosines)
        for j in range(nx):
            same = gx == j
            for x in range(planes):
                cosines[x] = jnp.where(same, xtab[scalars[3] + x, j], cosines[x])
                sines[x] = jnp.where(same, xtab[scalars[3] + x, nx + j], sines[x])
        block = i // per_block
        cols = pl.ds(pl.multiple_of((i - block * per_block) * TILE, TILE), TILE)
        for v in range(nv):
            re, im = 0.0, 0.0
            for x in range(planes):
                at = (v * planes + x) * 2 * bands
                sre, sim = acc[at : at + bands], acc[at + bands : at + 2 * bands]
                re = re + (sre * cosines[x] + sim * sines[x])
                im = im + (sim * cosines[x] - sre * sines[x])
            out[block % 2, v, block // 2, :, cols] = jnp.concatenate([re, im], 0)
        return 0

    lax.fori_loop(0, gvec.shape[1] // TILE, step, 0)


def pair_call(scalars, freq, cond_e, packed, cond, gvec, norm, slabs, count):
    bands, planes, ny, nz = cond.shape[1:]
    total = gvec.shape[1]
    nx = planes * slabs
    vm = pl.BlockSpec(memory_space=pltpu.VMEM)
    sm = pl.BlockSpec(memory_space=pltpu.SMEM)
    return pl.pallas_call(
        functools.partial(pair_kernel, float(count)),
        out_shape=(
            jax.ShapeDtypeStruct((2, 2, slabs // 2, 2 * bands, total // slabs), f32),
            jax.ShapeDtypeStruct((2, 2 * bands, 128), bf16),
        ),
        in_specs=[sm] * 4 + [vm] * 5,
        out_specs=(vm, vm),
        scratch_shapes=[pltpu.VMEM((ny, 2 * planes, 2 * bands, 2 * nz), bf16)],
        cost_estimate=pl.CostEstimate(flops=10**10, bytes_accessed=4 * 10**6, transcendentals=0),
        name="pairs",
    )(
        scalars,
        jnp.asarray(x_table(nx, norm)),
        freq,
        cond_e,
        packed,
        cond,
        gvec,
        jnp.asarray(y_table(bands, ny)),
        jnp.asarray(z_table(nz)),
    )


SIDE = 4
EXTRA = 128
CUT = 896


def response_kernel(freqs, row_g, part, wx, out, ga, gb, r1, s2, r2, rt, left, sel, send, recv, rsend, rrecv):
    ka = lax.axis_index("ka")
    slab = lax.axis_index("slab")
    zlo, core = slab // 2, slab % 2
    block_g = part.shape[4]
    xi, hi, yi = ka // 16, ka // 4 % 4, ka % 4

    def neighbour(axis, move):
        if axis == "x":
            return ((xi + move) % SIDE * 16 + hi * 4 + yi, slab)
        if axis == "h":
            return (xi * 16 + (hi + move) % SIDE * 4 + yi, slab)
        return (xi * 16 + hi * 4 + (yi + move) % SIDE, slab)

    peers = [(ka, (slab + d) % 4) for d in range(1, 4)]
    partner = (ka, zlo * 2 + 1 - core)
    across = (ka, (1 - zlo) * 2 + core)

    barrier = pltpu.get_barrier_semaphore()
    friends = [neighbour(axis, move) for axis in "xhy" for move in (1, 3)] + peers
    for friend in friends:
        pl.semaphore_signal(barrier, inc=1, device_id=friend, device_id_type=MESH)

    used = [0]
    sent = []

    def copy(src, dst, device):
        k = used[0]
        used[0] += 1
        c = pltpu.make_async_remote_copy(
            src_ref=src, dst_ref=dst, send_sem=send.at[k], recv_sem=recv.at[k],
            device_id=device, device_id_type=MESH,
        )
        sent.append(c)
        return c

    bufs = (ga, gb)
    inner, outer = ("x", "y"), ("y", "x")

    owner = ka * row_g // block_g
    at = ka * row_g - owner * block_g
    line = lax.broadcasted_iota(jnp.int32, sel.shape, 0)
    lane = lax.broadcasted_iota(jnp.int32, sel.shape, 1)
    target = jnp.where(line < row_g, line + at, line - row_g + block_g)
    sel[...] = (lane == target).astype(f32).astype(bf16)

    pl.semaphore_wait(barrier, len(friends))

    first = [copy(part.at[1 - core, v], r1.at[v], partner) for v in range(2)]
    for c in first:
        c.start()
    second = []
    for v in range(2):
        first[v].wait_recv()
        s2[v] = part[core, v, 1 - zlo] + r1[v, 1 - zlo]
        c = copy(s2.at[v], r2.at[v], across)
        c.start()
        second.append(c)

    class Ring:
        def __init__(self, axis, slots, low, high):
            self.axis, self.slots, self.low, self.high = axis, slots, low, high

        def start1(self):
            s, ax = self.slots, self.axis
            self.one = [copy(s(0), s(1), neighbour(ax, 1)), copy(s(0), s(2), neighbour(ax, 3))]
            for c in self.one:
                c.start()

        def turn(self):
            s, ax = self.slots, self.axis
            self.two = [
                copy(self.low(s(1)), self.low(s(3)), neighbour(ax, 1)),
                copy(self.high(s(2)), self.high(s(3)), neighbour(ax, 3)),
            ]
            for before, after in zip(self.one, self.two):
                before.wait_recv()
                after.start()

        def finish(self):
            for c in self.two:
                c.wait_recv()

    def lanes_low(ref):
        return ref.at[:, pl.ds(0, CUT)]

    def lanes_high(ref):
        return ref.at[:, pl.ds(CUT, block_g + EXTRA - CUT)]

    def make(v):
        g = bufs[v]
        tall = Ring("h", lambda j: g.at[j, 0, 0], lanes_low, lanes_high)
        ins = [Ring(inner[v], lambda j, h=h: g.at[h, 0, j], lanes_low, lanes_high) for h in range(4)]
        outs = [
            Ring(outer[v], lambda j, h=h: g.at[h, j], lambda r: r.at[pl.ds(0, 2)], lambda r: r.at[pl.ds(2, 2)])
            for h in range(4)
        ]
        return tall, ins, outs

    plan = [make(v) for v in range(2)]
    for v in range(2):
        tall, ins, outs = plan[v]
        mine = part[core, v, zlo] + r1[v, zlo]
        second[v].wait_recv()
        bufs[v][0, 0, 0, :, :block_g] = (mine + r2[v]).astype(bf16)
        bufs[v][0, 0, 0, :, block_g:] = wx[v]
        tall.start1()
        ins[0].start1()

    row_copies = []

    def ship_rows(chunk, v, h):
        copies = [
            pltpu.make_async_remote_copy(
                src_ref=rt.at[chunk], dst_ref=rt.at[chunk], send_sem=rsend.at[chunk, d],
                recv_sem=rrecv.at[chunk], device_id=peers[d], device_id_type=MESH,
            )
            for d in range(3)
        ]
        row_copies.append(copies)

        @pl.when(slab == owner)
        def _():
            held = bufs[v][h].reshape(256, block_g + EXTRA)
            picked = lax.dot_general(sel[...], held, (((1,), (1,)), ((), ())), preferred_element_type=f32)
            rt[chunk] = picked.astype(bf16)
            for c in copies:
                c.start()

    def multiply(chunk, v, h):
        @pl.when(slab != owner)
        def _():
            row_copies[chunk][0].wait_recv()

        both = rt[chunk].astype(f32)
        base = both[:row_g]
        spot = lax.broadcasted_iota(jnp.int32, base.shape, 1)
        swapped = jnp.where(spot % 16 < 8, pltpu.roll(base, 248, 1), -pltpu.roll(base, 8, 1))
        for w in range(freqs):
            k = row_g + 3 * w
            scale = both[k : k + 1] + both[k + 1 : k + 2] + both[k + 2 : k + 3]
            left[2 * w * row_g : (2 * w + 1) * row_g] = (base * scale).astype(bf16)
            left[(2 * w + 1) * row_g : (2 * w + 2) * row_g] = (swapped * scale).astype(bf16)

        def column(i, _):
            cols = pl.ds(pl.multiple_of(i * TILE, TILE), TILE)
            right = bufs[v][h, :, :, :, cols].reshape(256, TILE)
            product = jnp.dot(left[...], right, preferred_element_type=f32)
            if chunk == 0:
                out[:, cols] = product
            else:
                out[:, cols] += product
            return 0

        lax.fori_loop(0, block_g // TILE, column, 0)

    def each(action):
        for v in range(2):
            action(v, *plan[v])

    each(lambda v, tall, ins, outs: ins[0].turn())
    each(lambda v, tall, ins, outs: (tall.turn(), ins[1].start1(), ins[2].start1()))
    each(lambda v, tall, ins, outs: (ins[0].finish(), outs[0].start1()))
    each(lambda v, tall, ins, outs: (ins[1].turn(), ins[2].turn()))
    each(lambda v, tall, ins, outs: (tall.finish(), ins[3].start1()))
    each(lambda v, tall, ins, outs: (ins[1].finish(), outs[1].start1()))
    each(lambda v, tall, ins, outs: (ins[2].finish(), outs[2].start1()))
    each(lambda v, tall, ins, outs: ins[3].turn())
    each(lambda v, tall, ins, outs: outs[0].turn())
    each(lambda v, tall, ins, outs: (ins[3].finish(), outs[3].start1()))
    for h in range(4):
        for v in range(2):
            plan[v][2][h].finish()
            ship_rows(2 * h + v, v, h)
        if h < 3:
            each(lambda v, tall, ins, outs: outs[h + 1].turn())
        if h > 0:
            for v in range(2):
                multiply(2 * h - 2 + v, v, h - 1)
    for v in range(2):
        multiply(6 + v, v, 3)

    for c in sent:
        c.wait_send()

    @pl.when(slab == owner)
    def _():
        for copies in row_copies:
            for c in copies:
                c.wait_send()


def response_call(part, wx, freqs, row_g):
    half = part.shape[3]
    block_g = part.shape[4]
    wide = block_g + EXTRA
    tall = (row_g + 3 * freqs + 15) // 16 * 16
    vm = pl.BlockSpec(memory_space=pltpu.VMEM)
    rings = 4 + 2 * (4 + 16 + 16)
    return pl.pallas_call(
        functools.partial(response_kernel, freqs, row_g),
        out_shape=jax.ShapeDtypeStruct((freqs * 2 * row_g, block_g), f32),
        in_specs=[vm, vm],
        out_specs=vm,
        scratch_shapes=[
            pltpu.VMEM((4, 4, 4, half, wide), bf16),
            pltpu.VMEM((4, 4, 4, half, wide), bf16),
            pltpu.VMEM((2, 2, half, block_g), f32),
            pltpu.VMEM((2, half, block_g), f32),
            pltpu.VMEM((2, half, block_g), f32),
            pltpu.VMEM((8, tall, 256), bf16),
            pltpu.VMEM((freqs * 2 * row_g, 256), bf16),
            pltpu.VMEM((tall, wide), bf16),
            pltpu.SemaphoreType.DMA((rings,)),
            pltpu.SemaphoreType.DMA((rings,)),
            pltpu.SemaphoreType.DMA((8, 3)),
            pltpu.SemaphoreType.DMA((8,)),
        ],
        compiler_params=pltpu.CompilerParams(
            collective_id=0, has_side_effects=True, vmem_limit_bytes=48 * 1024 * 1024
        ),
        cost_estimate=pl.CostEstimate(flops=10**10, bytes_accessed=10**7, transcendentals=0),
        name="response",
    )(part, wx)


def shifted_target(index, shift, side):
    target = 0
    for stride in (side * side, side, 1):
        target += (index // stride + shift // stride) % side * stride
    return target


def route(payload, shift, side):
    count = side**3

    def along(offset):
        pairs = [(i, shifted_target(i, offset, side)) for i in range(count)]
        return lambda block: lax.ppermute(block, "ka", pairs)

    middle = shift // side % side
    outer = shift // (side * side) * side + shift % side
    ends = [i // side * side * side + i % side for i in range(1, side * side)]
    payload = lax.switch(middle, [lambda block: block] + [along(i * side) for i in range(1, side)], payload)
    return lax.switch(outer, [lambda block: block] + [along(i) for i in ends], payload)


def per_device(
    val_wave, cond_wave, val_energy, cond_energy, frequency, kpoint_map, umklapp, gvector_index
):
    slab_count = lax.axis_size("slab")
    kpoint_count = lax.axis_size("ka")
    here = lax.axis_index("ka")
    slab_here = lax.axis_index("slab")
    side = max((candidate for candidate in range(1, 9) if candidate**3 <= kpoint_count))
    shift = kpoint_map[0]
    planes, extent_y, extent_z = val_wave.shape[3:]
    fields = val_wave.shape[0] * val_wave.shape[2] * planes
    levels = jnp.pad(val_energy, ((0, extent_y - 1), (0, extent_z - val_energy.shape[1])))
    packed = jnp.concatenate([val_wave.reshape(fields, extent_y, extent_z), levels[None]], 0)
    packed = route(packed, shift, side)
    strides = [side * side, side, 1]
    wrapped = [(here // d % side < shift // d % side).astype(jnp.int32) for d in strides]
    scalars = jnp.stack(wrapped + [slab_here * planes]).astype(jnp.int32)
    points = planes * slab_count * extent_y * extent_z
    norm = 1.0 / (2.0 * math.sqrt(points))
    part, wx = pair_call(
        scalars, frequency, cond_energy, packed, cond_wave[:, 0], gvector_index[None], norm, slab_count, kpoint_count
    )
    freq_count = frequency.shape[0]
    total_g = gvector_index.shape[0]
    row_g = total_g // kpoint_count
    product = response_call(part, wx, freq_count, row_g)
    return product.reshape(freq_count, 2, row_g, total_g // slab_count)


def solution(mesh):
    return jax.shard_map(
        per_device,
        mesh=mesh,
        in_specs=(
            P(None, "ka", None, "slab", None, None),
            P(None, "ka", None, "slab", None, None),
            P("ka", None),
            P("ka", None),
            P(),
            P(),
            P(),
            P(),
        ),
        out_specs=P(None, None, "ka", "slab"),
        check_vma=False,
    )
```

```python
import functools
import math

import jax
import jax.numpy as jnp
import numpy as np
from jax import lax
from jax.experimental import pallas as pl
from jax.experimental.pallas import tpu as pltpu
from jax.sharding import PartitionSpec as P

HIGH = lax.Precision.HIGHEST
MESH = pl.DeviceIdType.MESH
f32, bf16 = jnp.float32, jnp.bfloat16
TILE = 512
SIDE = 4
CUT = 384
EXTRA = 128
ORDER = (
    "S0", "C00", "C01", "C02", "rs1_0", "C03", "S1", "C10", "C11", "fin_0", "Hs00", "Hs01", "Is000",
    "Is010", "C12", "rs1_1", "C13", "Itm000", "Itp000", "Itm010", "Itp010", "Htm00", "Htp00",
    "Is001", "Is002", "Htm01", "Htp01", "Is011", "Is012", "Os000", "Os010", "fin_1", "Hs10", "Hs11",
    "Is100", "Is110", "Itm001", "Itp001", "Itm002", "Itp002", "Is003", "Itm011", "Itp011", "Itm012",
    "Itp012", "Is013", "Otm010", "Otp010", "Itm100", "Itp100", "Htm10", "Htp10", "Is101", "Is102",
    "Otm000", "Otp000", "Os001", "Os002", "Itm110", "Itp110", "Os011", "Itm003", "Itp003", "Htm11",
    "Htp11", "Is111", "Is112", "Os012", "Itp013", "Itm013", "Os100", "R00", "Is103", "Itm101",
    "Itp101", "Itm102", "Itp102", "Is113", "Otm001", "Otp001", "Otm011", "Otp011", "Os003", "M00",
    "Itm111", "Itp111", "Itm112", "Itp112", "Otm002", "Otp002", "Os110", "Os013", "Otm012",
    "Otp012", "Itm103", "Itp103", "Os101", "Os102", "Otp100", "Otm100", "Itp113", "Itm113", "R01",
    "Otm110", "Otp110", "Otp003", "Otm003", "Os111", "Os112", "Otm013", "Otp013", "M01", "Os103",
    "R02", "Otp101", "Otm101", "Otp102", "Otm102", "Otm111", "Otp111", "R10", "Os113", "M02",
    "Otm112", "Otp112", "R03", "Otp103", "Otm103", "M10", "Otm113", "Otp113", "R11", "M03", "R12",
    "R13", "M11", "M12", "M13",
)


def y_table(bands, extent):
    index = np.arange(extent)
    angle = 2 * np.pi * (np.outer(index, index) % extent) / extent
    eye = np.eye(bands)
    size = bands * extent
    cos = np.einsum("ky,cd->kcdy", np.cos(angle), eye).reshape(size, size)
    sin = np.einsum("ky,cd->kcdy", np.sin(angle), eye).reshape(size, size)
    return np.block([[cos, sin], [-sin, cos]]).astype(np.float32)


def z_table(extent):
    index = np.arange(extent)
    angle = 2 * np.pi * (np.outer(index, index) % extent) / extent
    cos, sin = np.cos(angle), np.sin(angle)
    return np.block([[cos, -sin], [sin, cos]]).astype(np.float32)


def x_table(extent, norm):
    index = np.arange(extent)
    angle = 2 * np.pi * (np.outer(index, index) % extent) / extent
    return (np.concatenate([np.cos(angle), np.sin(angle)], 1) * norm).astype(np.float32)


def split_rows(value):
    high = value.astype(bf16)
    return high, (value - high.astype(f32)).astype(bf16)


def split_table(table, axis):
    high = table.astype(jnp.bfloat16)
    low = (table - high.astype(np.float32)).astype(jnp.bfloat16)
    return jnp.asarray(np.concatenate([high, high, low], axis))


def kernel(
    kpoints, row_g, shift, xtab, freq, cond_e, packed, cond, gvec, ytab, ztab, out,
    g00, g01, g10, g11, part, r1, s2, r2, spec, phase, wtile, rt, left, sel, wsel,
    send, recv, rsend, rrecv,
):
    ka = lax.axis_index("ka")
    slab = lax.axis_index("slab")
    zlo, core = slab // 2, slab % 2
    block_g = part.shape[3]
    half_g = block_g // 2
    freqs = freq.shape[0]
    coords = (ka // (SIDE * SIDE), ka // SIDE % SIDE, ka % SIDE)
    xi, hi, yi = coords
    bands, planes, ny, nz = cond.shape[1:]
    nv = 2
    nx = xtab.shape[0]
    rows = bands * ny
    height = planes * 2 * bands
    fields = nv * 2 * planes
    bufs = ((g00, g01), (g10, g11))

    def neighbour(axis, move):
        if axis == "x":
            return ((xi + move) % SIDE * 16 + hi * 4 + yi, slab)
        if axis == "h":
            return (xi * 16 + (hi + move) % SIDE * 4 + yi, slab)
        return (xi * 16 + hi * 4 + (yi + move) % SIDE, slab)

    peers = [(ka, (slab + d) % 4) for d in range(1, 4)]
    partner = (ka, zlo * 2 + 1 - core)
    across = (ka, (1 - zlo) * 2 + core)

    barrier = pltpu.get_barrier_semaphore()
    friends = [neighbour(axis, move) for axis in "xhy" for move in (1, 3)] + peers
    for friend in friends:
        pl.semaphore_signal(barrier, inc=1, device_id=friend, device_id_type=MESH)

    copies, waited = {}, set()

    def start(name, src, dst, device):
        k = len(copies)
        c = pltpu.make_async_remote_copy(
            src_ref=src, dst_ref=dst, send_sem=send.at[k], recv_sem=recv.at[k],
            device_id=device, device_id_type=MESH,
        )
        copies[name] = c
        c.start()

    def need(*names):
        for name in names:
            if name not in waited:
                waited.add(name)
                copies[name].wait_recv()

    q = shift[0]
    folds = [
        (coords[d] < q // SIDE ** (2 - d) % SIDE).astype(jnp.int32) for d in range(3)
    ]
    targets = [
        (1 - zlo) * 2 + 1 - core,
        (1 - zlo) * 2 + core,
        zlo * 2 + 1 - core,
        zlo * 2 + core,
    ]

    owner = ka * row_g // block_g
    at = ka * row_g - owner * block_g
    side_q = at // half_g
    line = lax.broadcasted_iota(jnp.int32, sel.shape, 0)
    lane = lax.broadcasted_iota(jnp.int32, sel.shape, 1)
    sel[...] = (lane == line + at - side_q * half_g).astype(f32).astype(bf16)
    for v in range(nv):
        line = lax.broadcasted_iota(jnp.int32, wsel.shape[1:], 0)
        lane = lax.broadcasted_iota(jnp.int32, wsel.shape[1:], 1)
        wsel[v] = ((lane == line + 3 * freqs * v) & (line < 3 * freqs)).astype(f32).astype(bf16)

    def weights():
        shape = (2 * bands, EXTRA)
        lane = lax.broadcasted_iota(jnp.int32, shape, 1)
        row = lax.broadcasted_iota(jnp.int32, shape, 0)
        level = jnp.zeros(shape, f32)
        for c in range(bands):
            level = jnp.where((row == c) | (row == bands + c), cond_e[0, c], level)
        omega = jnp.ones(shape, f32)
        value = jnp.zeros(shape, f32)
        for v in range(nv):
            for w in range(freqs):
                first = 3 * (v * freqs + w)
                omega = jnp.where((lane >= first) & (lane < first + 3), freq[w], omega)
        for v in range(nv):
            gap = packed[fields, 0:1, v : v + 1] - level
            weight = 2.0 * gap / (gap * gap + omega * omega) / kpoints
            high = weight.astype(bf16).astype(f32)
            mid = (weight - high).astype(bf16).astype(f32)
            low = weight - high - mid
            piece = lane % 3
            pieces = jnp.where(piece == 0, high, jnp.where(piece == 1, mid, low))
            first = 3 * v * freqs
            value = jnp.where((lane >= first) & (lane < first + 3 * freqs), pieces, value)
        wtile[...] = value.astype(bf16)

    def spectrum(v):
        columns = []
        for x in range(planes):
            vr = packed[v * planes + x][None]
            vi = packed[(nv + v) * planes + x][None]
            cr, ci = cond[0, :, x], cond[1, :, x]
            re = (vr * cr + vi * ci).reshape(rows, nz)
            im = (vr * ci - vi * cr).reshape(rows, nz)
            columns.append(jnp.concatenate([re, im], 0))
        high, low = split_rows(jnp.concatenate(columns, 1))
        t = jnp.dot(ytab[...], jnp.concatenate([high, low, high], 0), preferred_element_type=f32)
        t = [
            jnp.concatenate([t[:rows, x * nz : (x + 1) * nz], t[rows:, x * nz : (x + 1) * nz]], 1)
            for x in range(planes)
        ]
        high, low = split_rows(jnp.concatenate(t, 0))
        f = jnp.dot(jnp.concatenate([high, low, high], 1), ztab[...], preferred_element_type=f32)
        for x in range(planes):
            fx = f[x * rows : (x + 1) * rows]
            both = [fx[:, :nz].reshape(ny, bands, nz), fx[:, nz:].reshape(ny, bands, nz)]
            both = jnp.concatenate(both, 1).reshape(ny // 2, 2, 2 * bands, nz)
            for odd in range(2):
                high, low = split_rows(both[:, odd])
                here = slice(2 * bands * x, 2 * bands * (x + 1))
                spec[:, here, odd * nz : (odd + 1) * nz] = high
                spec[:, here, (2 + odd) * nz : (3 + odd) * nz] = low

    def columns_of(v, j):
        def step(i, _):
            cols = pl.ds(pl.multiple_of(targets[j] * block_g + i * TILE, TILE), TILE)
            local = pl.ds(pl.multiple_of(i * TILE, TILE), TILE)
            g = gvec[:, cols]
            gz = (g % nz - folds[2] + nz) % nz
            gy = (g // nz % ny - folds[1] + ny) % ny
            if v == 0:
                gx = g // (nz * ny) - folds[0]
                gx = jnp.where(gx < 0, gx + nx, gx)
                cosines = [jnp.zeros((1, TILE), f32) for _ in range(planes)]
                sines = list(cosines)
                for m in range(nx):
                    same = gx == m
                    for x in range(planes):
                        plane = slab * planes + x
                        cosines[x] = jnp.where(same, xtab[plane, m], cosines[x])
                        sines[x] = jnp.where(same, xtab[plane, nx + m], sines[x])
                for x in range(planes):
                    phase[x : x + 1, cols] = cosines[x]
                    phase[planes + x : planes + x + 1, cols] = sines[x]
            else:
                cosines = [phase[x : x + 1, cols] for x in range(planes)]
                sines = [phase[planes + x : planes + x + 1, cols] for x in range(planes)]
            code = gz + gy % 2 * nz
            hot = (lax.broadcasted_iota(jnp.int32, (2 * nz, TILE), 0) == code).astype(f32).astype(bf16)
            hot = jnp.concatenate([hot, hot], 0)
            table = spec[...].reshape(ny // 2 * height, 4 * nz)
            picked = jnp.dot(table, hot, preferred_element_type=f32)
            which = jnp.broadcast_to(gy // 2, (height, TILE))
            acc = picked[:height]
            for k in range(1, ny // 2):
                acc = jnp.where(which == k, picked[k * height : (k + 1) * height], acc)
            re, im = 0.0, 0.0
            for x in range(planes):
                a = x * 2 * bands
                sre, sim = acc[a : a + bands], acc[a + bands : a + 2 * bands]
                re = re + (sre * cosines[x] + sim * sines[x])
                im = im + (sim * cosines[x] - sre * sines[x])
            part[v, j, :, local] = jnp.concatenate([re, im], 0)
            return 0

        lax.fori_loop(0, block_g // TILE, step, 0)

    actions = {}

    def add(name, call):
        actions[name] = call

    def first_columns():
        columns_of(0, 0)
        pl.semaphore_wait(barrier, len(friends))
        start("ra0", part.at[0, 0], r1.at[0, 0], partner)

    def compute(v, j):
        if (v, j) == (0, 0):
            return first_columns
        if j % 2:
            return lambda: columns_of(v, j)

        def call():
            columns_of(v, j)
            name = ("ra", None, "rb")[j] + str(v)
            start(name, part.at[v, j], r1.at[v, j // 2], partner)

        return call

    def across_sum(v):
        def call():
            need(f"ra{v}")
            s2[v] = part[v, 1] + r1[v, 0]
            start(f"r2{v}", s2.at[v], r2.at[v], across)

        return call

    def finish_block(v):
        def call():
            need(f"rb{v}", f"r2{v}")
            total = (part[v, 3] + r1[v, 1] + r2[v]).astype(bf16)
            bufs[v][0][0, 0, 0] = total[:, :half_g]
            if v == 0:
                bufs[v][1][0, 0, 0, :, :half_g] = total[:, half_g:]
                bufs[v][1][0, 0, 0, :, half_g:] = wtile[...]
            else:
                bufs[v][1][0, 0, 0] = total[:, half_g:]

        return call

    def ring(one, two, names, axis, slots, low, high):
        def begin():
            start(one + "p", slots(0), slots(1), neighbour(axis, 1))
            start(one + "m", slots(0), slots(2), neighbour(axis, 3))

        def forward():
            need(one + "p")
            start(two + "p", low(slots(1)), low(slots(3)), neighbour(axis, 1))

        def back():
            need(one + "m")
            start(two + "m", high(slots(2)), high(slots(3)), neighbour(axis, 3))

        for name, call in zip(names, (begin, forward, back)):
            add(name, call)

    def after(events, name):
        inner_call = actions[name]

        def call():
            need(*events)
            inner_call()

        actions[name] = call

    def low_lanes(ref):
        return ref.at[:, pl.ds(0, CUT)]

    def high_lanes(ref):
        return ref.at[:, pl.ds(CUT, ref.shape[1] - CUT)]

    def low_blocks(ref):
        return ref.at[pl.ds(0, 2)]

    def high_blocks(ref):
        return ref.at[pl.ds(2, 2)]

    row_copies = {}

    def natural(v, side, h, cols):
        g = bufs[v][side]
        if side:
            return g[h, :, :, :, cols].reshape(SIDE * SIDE * 2 * bands, -1)
        return jnp.concatenate([g[h, y, x, :, cols] for x in range(SIDE) for y in range(SIDE)], 0)

    transposed = (((1,), (1,)), ((), ()))

    def ship_rows(v, h):
        chunk = v * SIDE + h

        def call():
            need(*[f"O{v}{side}{h}2{way}" for side in range(2) for way in "pm"])
            held = [
                pltpu.make_async_remote_copy(
                    src_ref=rt.at[chunk], dst_ref=rt.at[chunk], send_sem=rsend.at[chunk, d],
                    recv_sem=rrecv.at[chunk], device_id=peers[d], device_id_type=MESH,
                )
                for d in range(3)
            ]
            row_copies[chunk] = held

            @pl.when(slab == owner)
            def _():
                tiles = natural(0, 1, h, pl.ds(half_g, EXTRA))
                w = lax.dot_general(wsel[v], tiles, transposed, preferred_element_type=f32)
                rt[chunk, row_g:] = w.astype(bf16)
                for side in range(2):

                    @pl.when(side_q == side)
                    def _():
                        block = natural(v, side, h, pl.ds(0, half_g))
                        picked = lax.dot_general(sel[...], block, transposed, preferred_element_type=f32)
                        rt[chunk, :row_g] = picked.astype(bf16)

                for c in held:
                    c.start()

        return call

    def multiply(v, h):
        chunk = v * SIDE + h

        def call():
            @pl.when(slab != owner)
            def _():
                row_copies[chunk][0].wait_recv()

            both = rt[chunk].astype(f32)
            base = both[:row_g]
            spot = lax.broadcasted_iota(jnp.int32, base.shape, 1)
            swapped = jnp.where(spot % 16 < 8, pltpu.roll(base, 248, 1), -pltpu.roll(base, 8, 1))
            for w in range(freqs):
                k = row_g + 3 * w
                scale = both[k : k + 1] + both[k + 1 : k + 2] + both[k + 2 : k + 3]
                left[2 * w * row_g : (2 * w + 1) * row_g] = (base * scale).astype(bf16)
                left[(2 * w + 1) * row_g : (2 * w + 2) * row_g] = (swapped * scale).astype(bf16)
            for side in range(2):

                def column(i, _, side=side):
                    cols = pl.ds(pl.multiple_of(i * 256, 256), 256)
                    there = pl.ds(pl.multiple_of(side * half_g + i * 256, 256), 256)
                    product = jnp.dot(left[...], natural(v, side, h, cols), preferred_element_type=f32)
                    if chunk == 0:
                        out[:, there] = product
                    else:
                        out[:, there] += product
                    return 0

                lax.fori_loop(0, half_g // 256, column, 0)

        return call

    for v in range(nv):
        add(f"S{v}", lambda v=v: spectrum(v))
        for j in range(4):
            add(f"C{v}{j}", compute(v, j))
        add(f"rs1_{v}", across_sum(v))
        add(f"fin_{v}", finish_block(v))
        for side in range(2):
            g = bufs[v][side]
            k = f"{v}{side}"
            inner, outer = ("x", "y") if side == 0 else ("y", "x")
            ring(f"H{k}1", f"H{k}2", (f"Hs{k}", f"Htp{k}", f"Htm{k}"), "h",
                 lambda j, g=g: g.at[j, 0, 0], low_lanes, high_lanes)
            for h in range(SIDE):
                ring(f"I{k}{h}1", f"I{k}{h}2", (f"Is{k}{h}", f"Itp{k}{h}", f"Itm{k}{h}"), inner,
                     lambda j, g=g, h=h: g.at[h, 0, j], low_lanes, high_lanes)
                ring(f"O{k}{h}1", f"O{k}{h}2", (f"Os{k}{h}", f"Otp{k}{h}", f"Otm{k}{h}"), outer,
                     lambda j, g=g, h=h: g.at[h, j], low_blocks, high_blocks)
                before = ((), (f"H{k}1p",), (f"H{k}1m",), (f"H{k}2p", f"H{k}2m"))[h]
                after(before, f"Is{k}{h}")
                after([f"I{k}{h}{n}{way}" for n in "12" for way in "pm"], f"Os{k}{h}")
        for h in range(SIDE):
            add(f"R{v}{h}", ship_rows(v, h))
            add(f"M{v}{h}", multiply(v, h))

    weights()
    for name in ORDER:
        actions.pop(name)()
    assert not actions

    for c in copies.values():
        c.wait_send()

    @pl.when(slab == owner)
    def _():
        for held in row_copies.values():
            for c in held:
                c.wait_send()


def kernel_call(shift, freq, cond_e, packed, cond, gvec, norm, slabs, kpoints):
    bands, planes, ny, nz = cond.shape[1:]
    total = gvec.shape[1]
    nx = planes * slabs
    block_g, row_g, freqs = total // slabs, total // kpoints, freq.shape[0]
    half = 2 * bands
    tall = (row_g + 3 * freqs + 15) // 16 * 16
    vm = pl.BlockSpec(memory_space=pltpu.VMEM)
    sm = pl.BlockSpec(memory_space=pltpu.SMEM)
    count = 3 * 2 + 4 * (4 + 16 + 16)
    return pl.pallas_call(
        functools.partial(kernel, float(kpoints), row_g),
        out_shape=jax.ShapeDtypeStruct((freqs * 2 * row_g, block_g), f32),
        in_specs=[sm] * 4 + [vm] * 5,
        out_specs=vm,
        scratch_shapes=[
            pltpu.VMEM((4, 4, 4, half, block_g // 2), bf16),
            pltpu.VMEM((4, 4, 4, half, block_g // 2 + EXTRA), bf16),
            pltpu.VMEM((4, 4, 4, half, block_g // 2), bf16),
            pltpu.VMEM((4, 4, 4, half, block_g // 2), bf16),
            pltpu.VMEM((2, 4, half, block_g), f32),
            pltpu.VMEM((2, 2, half, block_g), f32),
            pltpu.VMEM((2, half, block_g), f32),
            pltpu.VMEM((2, half, block_g), f32),
            pltpu.VMEM((ny // 2, planes * half, 4 * nz), bf16),
            pltpu.VMEM((8, total), f32),
            pltpu.VMEM((half, EXTRA), bf16),
            pltpu.VMEM((8, tall, 256), bf16),
            pltpu.VMEM((freqs * 2 * row_g, 256), bf16),
            pltpu.VMEM((row_g, block_g // 2), bf16),
            pltpu.VMEM((2, tall - row_g, EXTRA), bf16),
            pltpu.SemaphoreType.DMA((count,)),
            pltpu.SemaphoreType.DMA((count,)),
            pltpu.SemaphoreType.DMA((8, 3)),
            pltpu.SemaphoreType.DMA((8,)),
        ],
        compiler_params=pltpu.CompilerParams(
            collective_id=0, has_side_effects=True, vmem_limit_bytes=48 * 1024 * 1024
        ),
        cost_estimate=pl.CostEstimate(flops=10**10, bytes_accessed=10**7, transcendentals=0),
        name="response",
    )(
        shift,
        jnp.asarray(x_table(nx, norm)),
        freq,
        cond_e,
        packed,
        cond,
        gvec,
        split_table(y_table(bands, ny), 1),
        split_table(z_table(nz), 0),
    )


def shifted_target(index, shift, side):
    target = 0
    for stride in (side * side, side, 1):
        target += (index // stride + shift // stride) % side * stride
    return target


def route(payload, shift, side):
    count = side**3

    def along(offset):
        pairs = [(i, shifted_target(i, offset, side)) for i in range(count)]
        return lambda block: lax.ppermute(block, "ka", pairs)

    middle = shift // side % side
    outer = shift // (side * side) * side + shift % side
    ends = [i // side * side * side + i % side for i in range(1, side * side)]
    payload = lax.switch(middle, [lambda block: block] + [along(i * side) for i in range(1, side)], payload)
    return lax.switch(outer, [lambda block: block] + [along(i) for i in ends], payload)


def per_device(
    val_wave, cond_wave, val_energy, cond_energy, frequency, kpoint_map, umklapp, gvector_index
):
    slab_count = lax.axis_size("slab")
    kpoint_count = lax.axis_size("ka")
    side = max((candidate for candidate in range(1, 9) if candidate**3 <= kpoint_count))
    shift = kpoint_map[0]
    planes, extent_y, extent_z = val_wave.shape[3:]
    fields = val_wave.shape[0] * val_wave.shape[2] * planes
    levels = jnp.pad(val_energy, ((0, extent_y - 1), (0, extent_z - val_energy.shape[1])))
    packed = jnp.concatenate([val_wave.reshape(fields, extent_y, extent_z), levels[None]], 0)
    packed = route(packed, shift, side)
    points = planes * slab_count * extent_y * extent_z
    norm = 1.0 / (2.0 * math.sqrt(points))
    freq_count = frequency.shape[0]
    total_g = gvector_index.shape[0]
    row_g = total_g // kpoint_count
    product = kernel_call(
        kpoint_map, frequency, cond_energy, packed, cond_wave[:, 0], gvector_index[None], norm,
        slab_count, kpoint_count,
    )
    return product.reshape(freq_count, 2, row_g, total_g // slab_count)


def solution(mesh):
    return jax.shard_map(
        per_device,
        mesh=mesh,
        in_specs=(
            P(None, "ka", None, "slab", None, None),
            P(None, "ka", None, "slab", None, None),
            P("ka", None),
            P("ka", None),
            P(),
            P(),
            P(),
            P(),
        ),
        out_specs=P(None, None, "ka", "slab"),
        check_vma=False,
    )
```

```python
import functools
import math

import jax
import jax.numpy as jnp
import numpy as np
from jax import lax
from jax.experimental import pallas as pl
from jax.experimental.pallas import tpu as pltpu
from jax.sharding import PartitionSpec as P

HIGH = lax.Precision.HIGHEST
MESH = pl.DeviceIdType.MESH
f32, bf16 = jnp.float32, jnp.bfloat16
TILE = 512
SIDE = 4
CUT = 384
EXTRA = 128
WIDE = 768
FIRST = 0
ORDER = (
    0, 1, 5, 9, 2, 6, 4, 10, 8, 3, 12, 7, 11, 13, 89, 90, 94, 98, 14, 15, 48, 18, 51, 21, 54, 91,
    93, 95, 97, 99, 101, 92, 96, 100, 102, 53, 20, 19, 52, 22, 23, 55, 56, 34, 17, 16, 27, 50, 49,
    60, 67, 24, 57, 103, 104, 137, 107, 140, 110, 143, 25, 58, 41, 36, 35, 37, 62, 61, 63, 29, 28,
    30, 69, 68, 70, 74, 26, 59, 145, 142, 141, 109, 108, 144, 112, 111, 106, 105, 116, 123, 43, 139,
    138, 149, 156, 42, 44, 38, 39, 64, 65, 32, 76, 31, 71, 130, 75, 77, 72, 81, 146, 163, 113, 114,
    147, 150, 152, 151, 119, 118, 117, 157, 159, 158, 124, 126, 125, 45, 46, 66, 82, 40, 73, 132,
    33, 165, 115, 131, 133, 148, 78, 164, 166, 79, 153, 47, 121, 160, 154, 128, 120, 85, 83, 161,
    127, 134, 170, 80, 135, 167, 168, 86, 122, 155, 84, 129, 162, 136, 171, 169, 87, 172, 174, 176,
    88, 173, 175, 177,
)


def y_table(bands, extent):
    index = np.arange(extent)
    angle = 2 * np.pi * (np.outer(index, index) % extent) / extent
    eye = np.eye(bands)
    size = bands * extent
    cos = np.einsum("ky,cd->kcdy", np.cos(angle), eye).reshape(size, size)
    sin = np.einsum("ky,cd->kcdy", np.sin(angle), eye).reshape(size, size)
    return np.block([[cos, sin], [-sin, cos]]).astype(np.float32)


def z_table(extent):
    index = np.arange(extent)
    angle = 2 * np.pi * (np.outer(index, index) % extent) / extent
    cos, sin = np.cos(angle), np.sin(angle)
    return np.block([[cos, -sin], [sin, cos]]).astype(np.float32)


def x_phases(extent, planes, norm):
    angle = 2 * np.pi * (np.outer(np.arange(planes), np.arange(extent)) % extent) / extent
    return np.cos(angle) * norm, np.sin(angle) * norm


def split_rows(value):
    high = value.astype(bf16)
    return high, (value - high.astype(f32)).astype(bf16)


def thrice(table, axis):
    high, low = jnp.split(table, 2, axis)
    return jnp.concatenate([high, high, low], axis)


def split_table(table, axis):
    high = table.astype(jnp.bfloat16)
    low = (table - high.astype(np.float32)).astype(jnp.bfloat16)
    return jnp.asarray(np.concatenate([high, low], axis))


def kernel(
    kpoints, row_g, norm, packed, shift_in, freq_in, cond_e_in, gvec_in, cond_in, ytab_in, ztab_in, out,
    g00, g01, g10, g11, part, r1, s2, r2, spec, phase, wtile, rt, left, sel, wsel,
    shift, freq, cond_e, cond, gvec, ytab, ztab, loads,
    send, recv, rsend, rrecv,
):
    inputs = (shift_in, freq_in, cond_e_in, gvec_in, cond_in, ytab_in, ztab_in)
    held_here = (shift, freq, cond_e, gvec, cond, ytab, ztab)
    fetches = [
        pltpu.make_async_copy(there, here, loads.at[i])
        for i, (there, here) in enumerate(zip(inputs, held_here))
    ]
    for fetch in fetches:
        fetch.start()
    ka = lax.axis_index("ka")
    slab = lax.axis_index("slab")
    zlo, core = slab // 2, slab % 2
    block_g = part.shape[3]
    half_g = block_g // 2
    freqs = freq.shape[0]
    coords = (ka // (SIDE * SIDE), ka // SIDE % SIDE, ka % SIDE)
    xi, hi, yi = coords
    bands, planes, ny, nz = cond.shape[1:]
    nv = 2
    nx = planes * 4
    rows = bands * ny
    height = planes * 2 * bands
    fields = nv * 2 * planes
    bufs = ((g00, g01), (g10, g11))

    def neighbour(axis, move):
        if axis == "x":
            return ((xi + move) % SIDE * 16 + hi * 4 + yi, slab)
        if axis == "h":
            return (xi * 16 + (hi + move) % SIDE * 4 + yi, slab)
        return (xi * 16 + hi * 4 + (yi + move) % SIDE, slab)

    peers = [(ka, (slab + d) % 4) for d in range(1, 4)]
    partner = (ka, zlo * 2 + 1 - core)
    across = (ka, (1 - zlo) * 2 + core)

    barrier = pltpu.get_barrier_semaphore()
    friends = [neighbour(axis, move) for axis in "xhy" for move in (1, 3)] + peers
    for friend in friends:
        pl.semaphore_signal(barrier, inc=1, device_id=friend, device_id_type=MESH)

    copies, waited = {}, set()

    def start(name, src, dst, device):
        k = len(copies)
        c = pltpu.make_async_remote_copy(
            src_ref=src, dst_ref=dst, send_sem=send.at[k], recv_sem=recv.at[k],
            device_id=device, device_id_type=MESH,
        )
        copies[name] = c
        c.start()

    def need(*names):
        for name in names:
            if name not in waited:
                waited.add(name)
                copies[name].wait_recv()

    for fetch in fetches:
        fetch.wait()

    q = shift[0]
    folds = [
        (coords[d] < q // SIDE ** (2 - d) % SIDE).astype(jnp.int32) for d in range(3)
    ]
    targets = [
        (1 - zlo) * 2 + 1 - core,
        (1 - zlo) * 2 + core,
        zlo * 2 + 1 - core,
        zlo * 2 + core,
    ]

    owner = ka * row_g // block_g
    at = ka * row_g - owner * block_g
    side_q = at // half_g
    line = lax.broadcasted_iota(jnp.int32, sel.shape, 0)
    lane = lax.broadcasted_iota(jnp.int32, sel.shape, 1)
    sel[...] = (lane == line + at - side_q * half_g).astype(f32).astype(bf16)
    for v in range(nv):
        line = lax.broadcasted_iota(jnp.int32, wsel.shape[1:], 0)
        lane = lax.broadcasted_iota(jnp.int32, wsel.shape[1:], 1)
        wsel[v] = ((lane == line + 3 * freqs * v) & (line < 3 * freqs)).astype(f32).astype(bf16)

    def weights():
        shape = (2 * bands, EXTRA)
        lane = lax.broadcasted_iota(jnp.int32, shape, 1)
        row = lax.broadcasted_iota(jnp.int32, shape, 0)
        level = jnp.zeros(shape, f32)
        for c in range(bands):
            level = jnp.where((row == c) | (row == bands + c), cond_e[0, c], level)
        omega = jnp.ones(shape, f32)
        value = jnp.zeros(shape, f32)
        for v in range(nv):
            for w in range(freqs):
                first = 3 * (v * freqs + w)
                omega = jnp.where((lane >= first) & (lane < first + 3), freq[w], omega)
        for v in range(nv):
            gap = packed[fields, 0:1, v : v + 1] - level
            weight = 2.0 * gap / (gap * gap + omega * omega) / kpoints
            high = weight.astype(bf16).astype(f32)
            mid = (weight - high).astype(bf16).astype(f32)
            low = weight - high - mid
            piece = lane % 3
            pieces = jnp.where(piece == 0, high, jnp.where(piece == 1, mid, low))
            first = 3 * v * freqs
            value = jnp.where((lane >= first) & (lane < first + 3 * freqs), pieces, value)
        wtile[...] = value.astype(bf16)

    def spectrum(v):
        columns = []
        for x in range(planes):
            vr = packed[v * planes + x][None]
            vi = packed[(nv + v) * planes + x][None]
            cr, ci = cond[0, :, x], cond[1, :, x]
            re = (vr * cr + vi * ci).reshape(rows, nz)
            im = (vr * ci - vi * cr).reshape(rows, nz)
            columns.append(jnp.concatenate([re, im], 0))
        high, low = split_rows(jnp.concatenate(columns, 1))
        t = jnp.dot(thrice(ytab[...], 1), jnp.concatenate([high, low, high], 0), preferred_element_type=f32)
        t = [
            jnp.concatenate([t[:rows, x * nz : (x + 1) * nz], t[rows:, x * nz : (x + 1) * nz]], 1)
            for x in range(planes)
        ]
        high, low = split_rows(jnp.concatenate(t, 0))
        f = jnp.dot(jnp.concatenate([high, low, high], 1), thrice(ztab[...], 0), preferred_element_type=f32)
        for x in range(planes):
            fx = f[x * rows : (x + 1) * rows]
            both = [fx[:, :nz].reshape(ny, bands, nz), fx[:, nz:].reshape(ny, bands, nz)]
            both = jnp.concatenate(both, 1).reshape(ny // 2, 2, 2 * bands, nz)
            for odd in range(2):
                high, low = split_rows(both[:, odd])
                here = slice(2 * bands * x, 2 * bands * (x + 1))
                spec[:, here, odd * nz : (odd + 1) * nz] = high
                spec[:, here, (2 + odd) * nz : (3 + odd) * nz] = low

    def columns_of(v, j, tile=None):
        def step(i, _):
            cols = pl.ds(pl.multiple_of(targets[j] * block_g + i * TILE, TILE), TILE)
            local = pl.ds(pl.multiple_of(i * TILE, TILE), TILE)
            g = gvec[:, cols]
            gz = (g % nz - folds[2] + nz) % nz
            gy = (g // nz % ny - folds[1] + ny) % ny
            if v == 0:
                gx = g // (nz * ny) - folds[0]
                gx = jnp.where(gx < 0, gx + nx, gx)
                turn = (slab * gx) % 4
                flip = turn % 2 == 1
                sign = jnp.where(turn >= 2, -1.0, 1.0)
                cos_of, sin_of = x_phases(nx, planes, norm)
                cosines, sines = [], []
                for x in range(planes):
                    c, s = jnp.full((1, TILE), norm, f32), jnp.zeros((1, TILE), f32)
                    for m in range(1, nx if x else 1):
                        c = jnp.where(gx == m, float(cos_of[x, m]), c)
                        s = jnp.where(gx == m, float(sin_of[x, m]), s)
                    cosines.append(sign * jnp.where(flip, -s, c))
                    sines.append(sign * jnp.where(flip, c, s))
                for x in range(planes):
                    phase[x : x + 1, cols] = cosines[x]
                    phase[planes + x : planes + x + 1, cols] = sines[x]
            else:
                cosines = [phase[x : x + 1, cols] for x in range(planes)]
                sines = [phase[planes + x : planes + x + 1, cols] for x in range(planes)]
            code = gz + gy % 2 * nz
            hot = (lax.broadcasted_iota(jnp.int32, (2 * nz, TILE), 0) == code).astype(f32).astype(bf16)
            hot = jnp.concatenate([hot, hot], 0)
            table = spec[...].reshape(ny // 2 * height, 4 * nz)
            picked = jnp.dot(table, hot, preferred_element_type=f32)
            which = jnp.broadcast_to(gy // 2, (height, TILE))
            acc = picked[:height]
            for k in range(1, ny // 2):
                acc = jnp.where(which == k, picked[k * height : (k + 1) * height], acc)
            re, im = 0.0, 0.0
            for x in range(planes):
                a = x * 2 * bands
                sre, sim = acc[a : a + bands], acc[a + bands : a + 2 * bands]
                re = re + (sre * cosines[x] + sim * sines[x])
                im = im + (sim * cosines[x] - sre * sines[x])
            part[v, j, :, local] = jnp.concatenate([re, im], 0)
            return 0

        if tile is not None:
            step(tile, 0)
        else:
            lax.fori_loop(0, block_g // TILE, step, 0)

    actions = {}

    def add(name, call):
        actions[name] = call

    def tile_cols(i):
        return pl.ds(i * TILE, TILE)

    def compute(v, j, i):
        def call():
            columns_of(v, j, i)
            if (v, j, i) == (0, 0, 0):
                pl.semaphore_wait(barrier, len(friends))
            if j == 0:
                here = part.at[v, 0, :, tile_cols(i)]
                start(f"ra{v}{i}", here, r1.at[v, 0, :, tile_cols(i)], partner)
            if j == 2 and i == block_g // TILE - 1:
                start(f"rb{v}", part.at[v, 2], r1.at[v, 1], partner)

        return call

    def across_sum(v, i):
        def call():
            need(f"ra{v}{i}")
            cols = tile_cols(i)
            s2[v, :, cols] = part[v, 1, :, cols] + r1[v, 0, :, cols]
            start(f"r2{v}{i}", s2.at[v, :, cols], r2.at[v, :, cols], across)

        return call

    def finish_block(v):
        def call():
            need(f"rb{v}", *[f"r2{v}{i}" for i in range(block_g // TILE)])
            total = (part[v, 3] + r1[v, 1] + r2[v]).astype(bf16)
            bufs[v][0][0, 0, 0] = total[:, :half_g]
            if v == 0:
                bufs[v][1][0, 0, 0, :, :half_g] = total[:, half_g:]
                bufs[v][1][0, 0, 0, :, half_g:] = wtile[...]
            else:
                bufs[v][1][0, 0, 0] = total[:, half_g:]

        return call

    def ring(one, two, names, axis, slots, low, high):
        def begin():
            start(one + "p", slots(0), slots(1), neighbour(axis, 1))
            start(one + "m", slots(0), slots(2), neighbour(axis, 3))

        def forward():
            need(one + "p")
            start(two + "p", low(slots(1)), low(slots(3)), neighbour(axis, 1))

        def back():
            need(one + "m")
            start(two + "m", high(slots(2)), high(slots(3)), neighbour(axis, 3))

        for name, call in zip(names, (begin, forward, back)):
            add(name, call)

    def after(events, name):
        inner_call = actions[name]

        def call():
            need(*events)
            inner_call()

        actions[name] = call

    def low_lanes(ref):
        return ref.at[:, pl.ds(0, CUT)]

    def high_lanes(ref):
        return ref.at[:, pl.ds(CUT, ref.shape[1] - CUT)]

    def low_blocks(ref):
        return ref.at[pl.ds(0, 2)]

    def high_blocks(ref):
        return ref.at[pl.ds(2, 2)]

    def units_of(h):
        if h == 0:
            return {"0": (0, 1), "1": (1, 1), "2": (2, 1), "3": (3, 1)}
        return {"a": (0, 2), "b": (2, 2)}

    def fine(v, side, h, axis):
        g = bufs[v][side]
        k = f"{v}{side}{h}"
        ready = ((), (f"I{k}1p",), (f"I{k}1m",), (f"I{k}2p", f"I{k}2m"))
        units = units_of(h)

        def begin(unit, first, count):
            def call():
                for i in range(first, first + count):
                    need(*ready[i])
                blocks = pl.ds(first, count)
                for way, slot, move in (("p", 1, 1), ("m", 2, 3)):
                    start(
                        f"O{k}{way}{unit}", g.at[h, 0, blocks], g.at[h, slot, blocks],
                        neighbour(axis, move),
                    )

            return call

        def turn(way, first, slot, move):
            def call():
                for unit, (at, count) in units.items():
                    if first <= at < first + 2:
                        need(f"O{k}{way}{unit}")
                blocks = pl.ds(first, 2)
                start(f"O{k}2{way}", g.at[h, slot, blocks], g.at[h, 3, blocks], neighbour(axis, move))

            return call

        for unit, (first, count) in units.items():
            add(f"Os{unit}{k}", begin(unit, first, count))
        add(f"Otp{k}", turn("p", 0, 1, 1))
        add(f"Otm{k}", turn("m", 2, 2, 3))

    row_copies = {}

    def natural(v, side, h, cols):
        g = bufs[v][side]
        if side:
            return g[h, :, :, :, cols].reshape(SIDE * SIDE * 2 * bands, -1)
        return jnp.concatenate([g[h, y, x, :, cols] for x in range(SIDE) for y in range(SIDE)], 0)

    transposed = (((1,), (1,)), ((), ()))

    def ship_rows(v, h):
        chunk = v * SIDE + h

        def call():
            for side in range(2):
                for way in "pm":
                    need(f"O{v}{side}{h}2{way}", *[f"O{v}{side}{h}{way}{u}" for u in units_of(h)])
                    need(f"O01{h}2{way}", *[f"O01{h}{way}{u}" for u in units_of(h)])
            held = [
                pltpu.make_async_remote_copy(
                    src_ref=rt.at[chunk], dst_ref=rt.at[chunk], send_sem=rsend.at[chunk, d],
                    recv_sem=rrecv.at[chunk], device_id=peers[d], device_id_type=MESH,
                )
                for d in range(3)
            ]
            row_copies[chunk] = held

            @pl.when(slab == owner)
            def _():
                tiles = natural(0, 1, h, pl.ds(half_g, EXTRA))
                w = lax.dot_general(wsel[v], tiles, transposed, preferred_element_type=f32)
                rt[chunk, row_g:] = w.astype(bf16)
                for side in range(2):

                    @pl.when(side_q == side)
                    def _():
                        block = natural(v, side, h, pl.ds(0, half_g))
                        picked = lax.dot_general(sel[...], block, transposed, preferred_element_type=f32)
                        rt[chunk, :row_g] = picked.astype(bf16)

                for c in held:
                    c.start()

        return call

    def multiply(v, h):
        chunk = v * SIDE + h

        def call():
            @pl.when(slab != owner)
            def _():
                row_copies[chunk][0].wait_recv()

            both = rt[chunk].astype(f32)
            base = both[:row_g]
            spot = lax.broadcasted_iota(jnp.int32, base.shape, 1)
            swapped = jnp.where(spot % 16 < 8, pltpu.roll(base, 248, 1), -pltpu.roll(base, 8, 1))
            for w in range(freqs):
                k = row_g + 3 * w
                scale = both[k : k + 1] + both[k + 1 : k + 2] + both[k + 2 : k + 3]
                left[2 * w * row_g : (2 * w + 1) * row_g] = (base * scale).astype(bf16)
                left[(2 * w + 1) * row_g : (2 * w + 2) * row_g] = (swapped * scale).astype(bf16)
            for side in range(2):

                def column(i, _, side=side):
                    cols = pl.ds(pl.multiple_of(i * WIDE, WIDE), WIDE)
                    there = pl.ds(pl.multiple_of(side * half_g + i * WIDE, WIDE), WIDE)
                    product = jnp.dot(left[...], natural(v, side, h, cols), preferred_element_type=f32)
                    if chunk == FIRST:
                        out[:, there] = product
                    else:
                        out[:, there] += product
                    return 0

                lax.fori_loop(0, half_g // WIDE, column, 0)

        return call

    for v in range(nv):
        add(f"S{v}", lambda v=v: spectrum(v))
        tiles = block_g // TILE
        for i in range(tiles):
            for j in range(3):
                add(f"T{v}{j}{i}", compute(v, j, i))
            add(f"rs{v}{i}", across_sum(v, i))
        add(f"C{v}3", lambda v=v: columns_of(v, 3))
        add(f"fin_{v}", finish_block(v))
        for side in range(2):
            g = bufs[v][side]
            k = f"{v}{side}"
            inner, outer = ("x", "y") if side == 0 else ("y", "x")
            ring(f"H{k}1", f"H{k}2", (f"Hs{k}", f"Htp{k}", f"Htm{k}"), "h",
                 lambda j, g=g: g.at[j, 0, 0], low_lanes, high_lanes)
            for h in range(SIDE):
                ring(f"I{k}{h}1", f"I{k}{h}2", (f"Is{k}{h}", f"Itp{k}{h}", f"Itm{k}{h}"), inner,
                     lambda j, g=g, h=h: g.at[h, 0, j], low_lanes, high_lanes)
                fine(v, side, h, outer)
                before = ((), (f"H{k}1p",), (f"H{k}1m",), (f"H{k}2p", f"H{k}2m"))[h]
                after(before, f"Is{k}{h}")
        for h in range(SIDE):
            add(f"R{v}{h}", ship_rows(v, h))
            add(f"M{v}{h}", multiply(v, h))

    weights()
    steps = list(actions.values())
    assert sorted(ORDER) == list(range(len(steps)))
    for at in ORDER:
        steps[at]()

    for c in copies.values():
        c.wait_send()

    @pl.when(slab == owner)
    def _():
        for held in row_copies.values():
            for c in held:
                c.wait_send()


def kernel_call(shift, freq, cond_e, packed, cond, gvec, norm, slabs, kpoints):
    bands, planes, ny, nz = cond.shape[1:]
    ytab, ztab = split_table(y_table(bands, ny), 1), split_table(z_table(nz), 0)
    fetched = (shift, freq, cond_e, gvec, cond, ytab, ztab)
    total = gvec.shape[1]
    block_g, row_g, freqs = total // slabs, total // kpoints, freq.shape[0]
    half = 2 * bands
    tall = (row_g + 3 * freqs + 15) // 16 * 16
    vm = pl.BlockSpec(memory_space=pltpu.VMEM)
    far = pl.BlockSpec(memory_space=pltpu.HBM)
    count = 2 * (3 + 1 + 3) + 4 * (4 + 16 + 10 + 3 * 6)
    return pl.pallas_call(
        functools.partial(kernel, float(kpoints), row_g, norm),
        out_shape=jax.ShapeDtypeStruct((freqs * 2 * row_g, block_g), f32),
        in_specs=[vm] + [far] * 7,
        out_specs=vm,
        scratch_shapes=[
            pltpu.VMEM((4, 4, 4, half, block_g // 2), bf16),
            pltpu.VMEM((4, 4, 4, half, block_g // 2 + EXTRA), bf16),
            pltpu.VMEM((4, 4, 4, half, block_g // 2), bf16),
            pltpu.VMEM((4, 4, 4, half, block_g // 2), bf16),
            pltpu.VMEM((2, 4, half, block_g), f32),
            pltpu.VMEM((2, 2, half, block_g), f32),
            pltpu.VMEM((2, half, block_g), f32),
            pltpu.VMEM((2, half, block_g), f32),
            pltpu.VMEM((ny // 2, planes * half, 4 * nz), bf16),
            pltpu.VMEM((8, total), f32),
            pltpu.VMEM((half, EXTRA), bf16),
            pltpu.VMEM((8, tall, 256), bf16),
            pltpu.VMEM((freqs * 2 * row_g, 256), bf16),
            pltpu.VMEM((row_g, block_g // 2), bf16),
            pltpu.VMEM((2, tall - row_g, EXTRA), bf16),
            pltpu.SMEM(shift.shape, jnp.int32),
            pltpu.SMEM(freq.shape, f32),
            pltpu.SMEM(cond_e.shape, f32),
            pltpu.VMEM(cond.shape, f32),
            pltpu.VMEM(gvec.shape, jnp.int32),
            pltpu.VMEM(ytab.shape, bf16),
            pltpu.VMEM(ztab.shape, bf16),
            pltpu.SemaphoreType.DMA((7,)),
            pltpu.SemaphoreType.DMA((count,)),
            pltpu.SemaphoreType.DMA((count,)),
            pltpu.SemaphoreType.DMA((8, 3)),
            pltpu.SemaphoreType.DMA((8,)),
        ],
        compiler_params=pltpu.CompilerParams(
            collective_id=0, has_side_effects=True, vmem_limit_bytes=46_000_000
        ),
        cost_estimate=pl.CostEstimate(flops=10**10, bytes_accessed=10**7, transcendentals=0),
        name="response",
    )(
        packed, *[pltpu.with_memory_space_constraint(a, pltpu.HBM) for a in fetched],
    )


def shifted_target(index, shift, side):
    target = 0
    for stride in (side * side, side, 1):
        target += (index // stride + shift // stride) % side * stride
    return target


def route(payload, shift, side):
    count = side**3

    def along(offset):
        pairs = [(i, shifted_target(i, offset, side)) for i in range(count)]
        return lambda block: lax.ppermute(block, "ka", pairs)

    middle = shift // side % side
    outer = shift // (side * side) * side + shift % side
    ends = [i // side * side * side + i % side for i in range(1, side * side)]
    payload = lax.switch(middle, [lambda block: block] + [along(i * side) for i in range(1, side)], payload)
    return lax.switch(outer, [lambda block: block] + [along(i) for i in ends], payload)


def per_device(
    val_wave, cond_wave, val_energy, cond_energy, frequency, kpoint_map, umklapp, gvector_index
):
    slab_count = lax.axis_size("slab")
    kpoint_count = lax.axis_size("ka")
    side = max((candidate for candidate in range(1, 9) if candidate**3 <= kpoint_count))
    shift = kpoint_map[0]
    planes, extent_y, extent_z = val_wave.shape[3:]
    fields = val_wave.shape[0] * val_wave.shape[2] * planes
    levels = jnp.pad(val_energy, ((0, extent_y - 1), (0, extent_z - val_energy.shape[1])))
    packed = jnp.concatenate([val_wave.reshape(fields, extent_y, extent_z), levels[None]], 0)
    packed = route(packed, shift, side)
    points = planes * slab_count * extent_y * extent_z
    norm = 1.0 / (2.0 * math.sqrt(points))
    freq_count = frequency.shape[0]
    total_g = gvector_index.shape[0]
    row_g = total_g // kpoint_count
    product = kernel_call(
        kpoint_map, frequency, cond_energy, packed, cond_wave[:, 0], gvector_index[None], norm,
        slab_count, kpoint_count,
    )
    return product.reshape(freq_count, 2, row_g, total_g // slab_count)


def solution(mesh):
    return jax.shard_map(
        per_device,
        mesh=mesh,
        in_specs=(
            P(None, "ka", None, "slab", None, None),
            P(None, "ka", None, "slab", None, None),
            P("ka", None),
            P("ka", None),
            P(),
            P(),
            P(),
            P(),
        ),
        out_specs=P(None, None, "ka", "slab"),
        check_vma=False,
    )
```

```python
import functools
import math

import jax
import jax.numpy as jnp
import numpy as np
from jax import lax
from jax.experimental import pallas as pl
from jax.experimental.pallas import tpu as pltpu
from jax.sharding import PartitionSpec as P

HIGH = lax.Precision.HIGHEST
MESH = pl.DeviceIdType.MESH
f32, bf16 = jnp.float32, jnp.bfloat16
TILE = 768
SIDE = 4
CUT = 384
EXTRA = 128
WIDE = 768
FIRST = 0
ORDER = (
    0, 1, 5, 2, 6, 4, 3, 8, 7, 9, 85, 86, 90, 87, 10, 14, 89, 11, 44, 47, 50, 17, 91, 93, 88, 92,
    94, 49, 15, 16, 48, 18, 19, 52, 51, 30, 13, 23, 12, 63, 46, 20, 53, 21, 45, 56, 95, 96, 99, 129,
    132, 102, 135, 54, 31, 32, 33, 25, 26, 24, 65, 66, 64, 55, 22, 37, 58, 101, 100, 104, 103, 134,
    137, 70, 57, 59, 98, 115, 133, 136, 97, 108, 34, 27, 131, 148, 130, 141, 35, 68, 28, 38, 39, 40,
    67, 105, 77, 122, 106, 71, 73, 61, 60, 155, 138, 117, 72, 116, 118, 139, 110, 109, 36, 111, 78,
    149, 150, 142, 29, 124, 151, 41, 144, 69, 143, 123, 125, 107, 157, 75, 62, 140, 42, 74, 156,
    158, 119, 120, 112, 81, 113, 152, 153, 43, 79, 145, 146, 126, 127, 162, 76, 82, 121, 159, 80,
    154, 160, 114, 147, 163, 128, 83, 161, 166, 164, 168, 84, 167, 165, 169,
)


def y_table(bands, extent):
    index = np.arange(extent)
    angle = 2 * np.pi * (np.outer(index, index) % extent) / extent
    eye = np.eye(bands)
    size = bands * extent
    cos = np.einsum("ky,cd->kcdy", np.cos(angle), eye).reshape(size, size)
    sin = np.einsum("ky,cd->kcdy", np.sin(angle), eye).reshape(size, size)
    return np.block([[cos, sin], [-sin, cos]]).astype(np.float32)


def z_table(extent):
    index = np.arange(extent)
    angle = 2 * np.pi * (np.outer(index, index) % extent) / extent
    cos, sin = np.cos(angle), np.sin(angle)
    return np.block([[cos, -sin], [sin, cos]]).astype(np.float32)


def x_phases(extent, planes, norm):
    angle = 2 * np.pi * (np.outer(np.arange(planes), np.arange(extent)) % extent) / extent
    return np.cos(angle) * norm, np.sin(angle) * norm


def split_rows(value):
    high = value.astype(bf16)
    return high, (value - high.astype(f32)).astype(bf16)


def thrice(table, axis):
    high, low = jnp.split(table, 2, axis)
    return jnp.concatenate([high, high, low], axis)


def split_table(table, axis):
    high = table.astype(jnp.bfloat16)
    low = (table - high.astype(np.float32)).astype(jnp.bfloat16)
    return jnp.asarray(np.concatenate([high, low], axis))


def kernel(
    kpoints, row_g, norm, packed, shift_in, freq_in, cond_e_in, gvec_in, cond_in, ytab_in, ztab_in, out,
    g00, g01, g10, g11, part, r1, s2, r2, spec, phase, wtile, rt, left, sel, wsel,
    shift, freq, cond_e, cond, gvec, ytab, ztab, counter, loads,
    send, recv, rsend, rrecv,
):
    inputs = (shift_in, freq_in, cond_e_in, gvec_in, cond_in, ytab_in, ztab_in)
    held_here = (shift, freq, cond_e, gvec, cond, ytab, ztab)
    fetches = [
        pltpu.make_async_copy(there, here, loads.at[i])
        for i, (there, here) in enumerate(zip(inputs, held_here))
    ]
    for fetch in fetches:
        fetch.start()
    ka = lax.axis_index("ka")
    slab = lax.axis_index("slab")
    zlo, core = slab // 2, slab % 2
    block_g = part.shape[3]
    half_g = block_g // 2
    freqs = freq.shape[0]
    coords = (ka // (SIDE * SIDE), ka // SIDE % SIDE, ka % SIDE)
    xi, hi, yi = coords
    bands, planes, ny, nz = cond.shape[1:]
    nv = 2
    nx = planes * 4
    rows = bands * ny
    height = planes * 2 * bands
    fields = nv * 2 * planes
    bufs = ((g00, g01), (g10, g11))

    def neighbour(axis, move):
        if axis == "x":
            return ((xi + move) % SIDE * 16 + hi * 4 + yi, slab)
        if axis == "h":
            return (xi * 16 + (hi + move) % SIDE * 4 + yi, slab)
        return (xi * 16 + hi * 4 + (yi + move) % SIDE, slab)

    peers = [(ka, (slab + d) % 4) for d in range(1, 4)]
    partner = (ka, zlo * 2 + 1 - core)
    across = (ka, (1 - zlo) * 2 + core)

    barrier = pltpu.get_barrier_semaphore()
    friends = [neighbour(axis, move) for axis in "xhy" for move in (1, 3)] + peers
    for friend in friends:
        pl.semaphore_signal(barrier, inc=1, device_id=friend, device_id_type=MESH)

    copies, waited = {}, set()

    def start(name, src, dst, device):
        k = len(copies)
        c = pltpu.make_async_remote_copy(
            src_ref=src, dst_ref=dst, send_sem=send.at[k], recv_sem=recv.at[k],
            device_id=device, device_id_type=MESH,
        )
        copies[name] = c
        c.start()

    def need(*names):
        for name in names:
            if name not in waited:
                waited.add(name)
                copies[name].wait_recv()

    for fetch in fetches:
        fetch.wait()

    q = shift[0]
    folds = [
        (coords[d] < q // SIDE ** (2 - d) % SIDE).astype(jnp.int32) for d in range(3)
    ]
    targets = [
        (1 - zlo) * 2 + 1 - core,
        (1 - zlo) * 2 + core,
        zlo * 2 + 1 - core,
        zlo * 2 + core,
    ]

    owner = ka * row_g // block_g
    at = ka * row_g - owner * block_g
    side_q = at // half_g
    line = lax.broadcasted_iota(jnp.int32, sel.shape, 0)
    lane = lax.broadcasted_iota(jnp.int32, sel.shape, 1)
    sel[...] = (lane == line + at - side_q * half_g).astype(f32).astype(bf16)
    for v in range(nv):
        line = lax.broadcasted_iota(jnp.int32, wsel.shape[1:], 0)
        lane = lax.broadcasted_iota(jnp.int32, wsel.shape[1:], 1)
        wsel[v] = ((lane == line + 3 * freqs * v) & (line < 3 * freqs)).astype(f32).astype(bf16)

    def weights():
        shape = (2 * bands, EXTRA)
        lane = lax.broadcasted_iota(jnp.int32, shape, 1)
        row = lax.broadcasted_iota(jnp.int32, shape, 0)
        level = jnp.zeros(shape, f32)
        for c in range(bands):
            level = jnp.where((row == c) | (row == bands + c), cond_e[0, c], level)
        omega = jnp.ones(shape, f32)
        value = jnp.zeros(shape, f32)
        for v in range(nv):
            for w in range(freqs):
                first = 3 * (v * freqs + w)
                omega = jnp.where((lane >= first) & (lane < first + 3), freq[w], omega)
        for v in range(nv):
            gap = packed[fields, 0:1, v : v + 1] - level
            weight = 2.0 * gap / (gap * gap + omega * omega) / kpoints
            high = weight.astype(bf16).astype(f32)
            mid = (weight - high).astype(bf16).astype(f32)
            low = weight - high - mid
            piece = lane % 3
            pieces = jnp.where(piece == 0, high, jnp.where(piece == 1, mid, low))
            first = 3 * v * freqs
            value = jnp.where((lane >= first) & (lane < first + 3 * freqs), pieces, value)
        wtile[...] = value.astype(bf16)

    def spectrum(v):
        columns = []
        for x in range(planes):
            vr = packed[v * planes + x][None]
            vi = packed[(nv + v) * planes + x][None]
            cr, ci = cond[0, :, x], cond[1, :, x]
            re = (vr * cr + vi * ci).reshape(rows, nz)
            im = (vr * ci - vi * cr).reshape(rows, nz)
            columns.append(jnp.concatenate([re, im], 0))
        high, low = split_rows(jnp.concatenate(columns, 1))
        t = jnp.dot(thrice(ytab[...], 1), jnp.concatenate([high, low, high], 0), preferred_element_type=f32)
        t = [
            jnp.concatenate([t[:rows, x * nz : (x + 1) * nz], t[rows:, x * nz : (x + 1) * nz]], 1)
            for x in range(planes)
        ]
        high, low = split_rows(jnp.concatenate(t, 0))
        f = jnp.dot(jnp.concatenate([high, low, high], 1), thrice(ztab[...], 0), preferred_element_type=f32)
        for x in range(planes):
            fx = f[x * rows : (x + 1) * rows]
            both = [fx[:, :nz].reshape(ny, bands, nz), fx[:, nz:].reshape(ny, bands, nz)]
            both = jnp.concatenate(both, 1).reshape(ny // 2, 2, 2 * bands, nz)
            for odd in range(2):
                high, low = split_rows(both[:, odd])
                here = slice(2 * bands * x, 2 * bands * (x + 1))
                spec[:, here, odd * nz : (odd + 1) * nz] = high
                spec[:, here, (2 + odd) * nz : (3 + odd) * nz] = low

    def columns_of(v, j, tile=None):
        def step(i, _):
            cols = pl.ds(pl.multiple_of(targets[j] * block_g + i * TILE, TILE), TILE)
            local = pl.ds(pl.multiple_of(i * TILE, TILE), TILE)
            g = gvec[:, cols]
            gz = (g - folds[2] + nz) & (nz - 1)
            gy = ((g >> 7) - folds[1] + ny) & (ny - 1)
            if v == 0:
                gx = (g >> 11) - folds[0]
                gx = jnp.where(gx < 0, gx + nx, gx)
                turn = (slab * gx) & 3
                flip = (turn & 1) == 1
                sign = jnp.where(turn >= 2, -1.0, 1.0)
                cos_of, sin_of = x_phases(nx, planes, norm)
                cosines, sines = [], []
                for x in range(planes):
                    c, s = jnp.full((1, TILE), norm, f32), jnp.zeros((1, TILE), f32)
                    for m in range(1, nx if x else 1):
                        c = jnp.where(gx == m, float(cos_of[x, m]), c)
                        s = jnp.where(gx == m, float(sin_of[x, m]), s)
                    cosines.append(sign * jnp.where(flip, -s, c))
                    sines.append(sign * jnp.where(flip, c, s))
                for x in range(planes):
                    phase[x : x + 1, cols] = cosines[x]
                    phase[planes + x : planes + x + 1, cols] = sines[x]
            else:
                cosines = [phase[x : x + 1, cols] for x in range(planes)]
                sines = [phase[planes + x : planes + x + 1, cols] for x in range(planes)]
            code = gz + (gy & 1) * nz
            same = counter[...] == jnp.broadcast_to(code.astype(f32).astype(bf16), counter.shape)
            hot = jnp.where(same, jnp.ones(counter.shape, bf16), jnp.zeros(counter.shape, bf16))
            hot = jnp.concatenate([hot, hot], 0)
            table = spec[...].reshape(ny // 2 * height, 4 * nz)
            picked = jnp.dot(table, hot, preferred_element_type=f32)
            which = jnp.broadcast_to(gy >> 1, (height, TILE))
            acc = picked[:height]
            for k in range(1, ny // 2):
                acc = jnp.where(which == k, picked[k * height : (k + 1) * height], acc)
            re, im = 0.0, 0.0
            for x in range(planes):
                a = x * 2 * bands
                sre, sim = acc[a : a + bands], acc[a + bands : a + 2 * bands]
                re = re + (sre * cosines[x] + sim * sines[x])
                im = im + (sim * cosines[x] - sre * sines[x])
            part[v, j, :, local] = jnp.concatenate([re, im], 0)
            return 0

        if tile is not None:
            step(tile, 0)
        else:
            lax.fori_loop(0, block_g // TILE, step, 0)

    actions = {}

    def add(name, call):
        actions[name] = call

    def tile_cols(i):
        return pl.ds(i * TILE, TILE)

    def compute(v, j, i):
        def call():
            columns_of(v, j, i)
            if (v, j, i) == (0, 0, 0):
                pl.semaphore_wait(barrier, len(friends))
            if j == 0:
                here = part.at[v, 0, :, tile_cols(i)]
                start(f"ra{v}{i}", here, r1.at[v, 0, :, tile_cols(i)], partner)
            if j == 2 and i == block_g // TILE - 1:
                start(f"rb{v}", part.at[v, 2], r1.at[v, 1], partner)

        return call

    def across_sum(v, i):
        def call():
            need(f"ra{v}{i}")
            cols = tile_cols(i)
            s2[v, :, cols] = part[v, 1, :, cols] + r1[v, 0, :, cols]
            start(f"r2{v}{i}", s2.at[v, :, cols], r2.at[v, :, cols], across)

        return call

    def finish_block(v):
        def call():
            need(f"rb{v}", *[f"r2{v}{i}" for i in range(block_g // TILE)])
            total = (part[v, 3] + r1[v, 1] + r2[v]).astype(bf16)
            bufs[v][0][0, 0, 0] = total[:, :half_g]
            if v == 0:
                bufs[v][1][0, 0, 0, :, :half_g] = total[:, half_g:]
                bufs[v][1][0, 0, 0, :, half_g:] = wtile[...]
            else:
                bufs[v][1][0, 0, 0] = total[:, half_g:]

        return call

    def ring(one, two, names, axis, slots, low, high):
        def begin():
            start(one + "p", slots(0), slots(1), neighbour(axis, 1))
            start(one + "m", slots(0), slots(2), neighbour(axis, 3))

        def forward():
            need(one + "p")
            start(two + "p", low(slots(1)), low(slots(3)), neighbour(axis, 1))

        def back():
            need(one + "m")
            start(two + "m", high(slots(2)), high(slots(3)), neighbour(axis, 3))

        for name, call in zip(names, (begin, forward, back)):
            add(name, call)

    def after(events, name):
        inner_call = actions[name]

        def call():
            need(*events)
            inner_call()

        actions[name] = call

    def low_lanes(ref):
        return ref.at[:, pl.ds(0, CUT)]

    def high_lanes(ref):
        return ref.at[:, pl.ds(CUT, ref.shape[1] - CUT)]

    def low_blocks(ref):
        return ref.at[pl.ds(0, 2)]

    def high_blocks(ref):
        return ref.at[pl.ds(2, 2)]

    def units_of(h):
        if h == 0:
            return {"0": (0, 1), "1": (1, 1), "2": (2, 1), "3": (3, 1)}
        return {"a": (0, 2), "b": (2, 2)}

    def fine(v, side, h, axis):
        g = bufs[v][side]
        k = f"{v}{side}{h}"
        ready = ((), (f"I{k}1p",), (f"I{k}1m",), (f"I{k}2p", f"I{k}2m"))
        units = units_of(h)

        def begin(unit, first, count):
            def call():
                for i in range(first, first + count):
                    need(*ready[i])
                blocks = pl.ds(first, count)
                for way, slot, move in (("p", 1, 1), ("m", 2, 3)):
                    start(
                        f"O{k}{way}{unit}", g.at[h, 0, blocks], g.at[h, slot, blocks],
                        neighbour(axis, move),
                    )

            return call

        def turn(way, first, slot, move):
            def call():
                for unit, (at, count) in units.items():
                    if first <= at < first + 2:
                        need(f"O{k}{way}{unit}")
                blocks = pl.ds(first, 2)
                start(f"O{k}2{way}", g.at[h, slot, blocks], g.at[h, 3, blocks], neighbour(axis, move))

            return call

        for unit, (first, count) in units.items():
            add(f"Os{unit}{k}", begin(unit, first, count))
        add(f"Otp{k}", turn("p", 0, 1, 1))
        add(f"Otm{k}", turn("m", 2, 2, 3))

    row_copies = {}

    def natural(v, side, h, cols):
        g = bufs[v][side]
        if side:
            return g[h, :, :, :, cols].reshape(SIDE * SIDE * 2 * bands, -1)
        return jnp.concatenate([g[h, y, x, :, cols] for x in range(SIDE) for y in range(SIDE)], 0)

    transposed = (((1,), (1,)), ((), ()))

    def ship_rows(v, h):
        chunk = v * SIDE + h

        def call():
            for side in range(2):
                for way in "pm":
                    need(f"O{v}{side}{h}2{way}", *[f"O{v}{side}{h}{way}{u}" for u in units_of(h)])
                    need(f"O01{h}2{way}", *[f"O01{h}{way}{u}" for u in units_of(h)])
            held = [
                pltpu.make_async_remote_copy(
                    src_ref=rt.at[chunk], dst_ref=rt.at[chunk], send_sem=rsend.at[chunk, d],
                    recv_sem=rrecv.at[chunk], device_id=peers[d], device_id_type=MESH,
                )
                for d in range(3)
            ]
            row_copies[chunk] = held

            @pl.when(slab == owner)
            def _():
                tiles = natural(0, 1, h, pl.ds(half_g, EXTRA))
                w = lax.dot_general(wsel[v], tiles, transposed, preferred_element_type=f32)
                rt[chunk, row_g:] = w.astype(bf16)
                for side in range(2):

                    @pl.when(side_q == side)
                    def _():
                        block = natural(v, side, h, pl.ds(0, half_g))
                        picked = lax.dot_general(sel[...], block, transposed, preferred_element_type=f32)
                        rt[chunk, :row_g] = picked.astype(bf16)

                for c in held:
                    c.start()

        return call

    def multiply(v, h):
        chunk = v * SIDE + h

        def call():
            @pl.when(slab != owner)
            def _():
                row_copies[chunk][0].wait_recv()

            both = rt[chunk].astype(f32)
            base = both[:row_g]
            spot = lax.broadcasted_iota(jnp.int32, base.shape, 1)
            swapped = jnp.where(spot % 16 < 8, pltpu.roll(base, 248, 1), -pltpu.roll(base, 8, 1))
            for w in range(freqs):
                k = row_g + 3 * w
                scale = both[k : k + 1] + both[k + 1 : k + 2] + both[k + 2 : k + 3]
                left[2 * w * row_g : (2 * w + 1) * row_g] = (base * scale).astype(bf16)
                left[(2 * w + 1) * row_g : (2 * w + 2) * row_g] = (swapped * scale).astype(bf16)
            for side in range(2):

                def column(i, _, side=side):
                    cols = pl.ds(pl.multiple_of(i * WIDE, WIDE), WIDE)
                    there = pl.ds(pl.multiple_of(side * half_g + i * WIDE, WIDE), WIDE)
                    product = jnp.dot(left[...], natural(v, side, h, cols), preferred_element_type=f32)
                    if chunk == FIRST:
                        out[:, there] = product
                    else:
                        out[:, there] += product
                    return 0

                lax.fori_loop(0, half_g // WIDE, column, 0)

        return call

    for v in range(nv):
        add(f"S{v}", lambda v=v: spectrum(v))
        tiles = block_g // TILE
        for i in range(tiles):
            for j in range(3):
                add(f"T{v}{j}{i}", compute(v, j, i))
            add(f"rs{v}{i}", across_sum(v, i))
        add(f"C{v}3", lambda v=v: columns_of(v, 3))
        add(f"fin_{v}", finish_block(v))
        for side in range(2):
            g = bufs[v][side]
            k = f"{v}{side}"
            inner, outer = ("x", "y") if side == 0 else ("y", "x")
            ring(f"H{k}1", f"H{k}2", (f"Hs{k}", f"Htp{k}", f"Htm{k}"), "h",
                 lambda j, g=g: g.at[j, 0, 0], low_lanes, high_lanes)
            for h in range(SIDE):
                ring(f"I{k}{h}1", f"I{k}{h}2", (f"Is{k}{h}", f"Itp{k}{h}", f"Itm{k}{h}"), inner,
                     lambda j, g=g, h=h: g.at[h, 0, j], low_lanes, high_lanes)
                fine(v, side, h, outer)
                before = ((), (f"H{k}1p",), (f"H{k}1m",), (f"H{k}2p", f"H{k}2m"))[h]
                after(before, f"Is{k}{h}")
        for h in range(SIDE):
            add(f"R{v}{h}", ship_rows(v, h))
            add(f"M{v}{h}", multiply(v, h))

    counter[...] = lax.broadcasted_iota(jnp.int32, counter.shape, 0).astype(f32).astype(bf16)
    weights()
    steps = list(actions.values())
    assert sorted(ORDER) == list(range(len(steps)))
    for at in ORDER:
        steps[at]()

    for c in copies.values():
        c.wait_send()

    @pl.when(slab == owner)
    def _():
        for held in row_copies.values():
            for c in held:
                c.wait_send()


def kernel_call(shift, freq, cond_e, packed, cond, gvec, norm, slabs, kpoints):
    bands, planes, ny, nz = cond.shape[1:]
    ytab, ztab = split_table(y_table(bands, ny), 1), split_table(z_table(nz), 0)
    fetched = (shift, freq, cond_e, gvec, cond, ytab, ztab)
    total = gvec.shape[1]
    block_g, row_g, freqs = total // slabs, total // kpoints, freq.shape[0]
    half = 2 * bands
    tall = (row_g + 3 * freqs + 15) // 16 * 16
    vm = pl.BlockSpec(memory_space=pltpu.VMEM)
    far = pl.BlockSpec(memory_space=pltpu.HBM)
    count = 2 * (3 + 1 + 3) + 4 * (4 + 16 + 10 + 3 * 6)
    return pl.pallas_call(
        functools.partial(kernel, float(kpoints), row_g, norm),
        out_shape=jax.ShapeDtypeStruct((freqs * 2 * row_g, block_g), f32),
        in_specs=[vm] + [far] * 7,
        out_specs=vm,
        scratch_shapes=[
            pltpu.VMEM((4, 4, 4, half, block_g // 2), bf16),
            pltpu.VMEM((4, 4, 4, half, block_g // 2 + EXTRA), bf16),
            pltpu.VMEM((4, 4, 4, half, block_g // 2), bf16),
            pltpu.VMEM((4, 4, 4, half, block_g // 2), bf16),
            pltpu.VMEM((2, 4, half, block_g), f32),
            pltpu.VMEM((2, 2, half, block_g), f32),
            pltpu.VMEM((2, half, block_g), f32),
            pltpu.VMEM((2, half, block_g), f32),
            pltpu.VMEM((ny // 2, planes * half, 4 * nz), bf16),
            pltpu.VMEM((8, total), f32),
            pltpu.VMEM((half, EXTRA), bf16),
            pltpu.VMEM((8, tall, 256), bf16),
            pltpu.VMEM((freqs * 2 * row_g, 256), bf16),
            pltpu.VMEM((row_g, block_g // 2), bf16),
            pltpu.VMEM((2, tall - row_g, EXTRA), bf16),
            pltpu.SMEM(shift.shape, jnp.int32),
            pltpu.SMEM(freq.shape, f32),
            pltpu.SMEM(cond_e.shape, f32),
            pltpu.VMEM(cond.shape, f32),
            pltpu.VMEM(gvec.shape, jnp.int32),
            pltpu.VMEM(ytab.shape, bf16),
            pltpu.VMEM(ztab.shape, bf16),
            pltpu.VMEM((2 * nz, TILE), bf16),
            pltpu.SemaphoreType.DMA((7,)),
            pltpu.SemaphoreType.DMA((count,)),
            pltpu.SemaphoreType.DMA((count,)),
            pltpu.SemaphoreType.DMA((8, 3)),
            pltpu.SemaphoreType.DMA((8,)),
        ],
        compiler_params=pltpu.CompilerParams(
            collective_id=0, has_side_effects=True, vmem_limit_bytes=46_000_000
        ),
        cost_estimate=pl.CostEstimate(flops=10**10, bytes_accessed=10**7, transcendentals=0),
        name="response",
    )(
        packed, *[pltpu.with_memory_space_constraint(a, pltpu.HBM) for a in fetched],
    )


def shifted_target(index, shift, side):
    target = 0
    for stride in (side * side, side, 1):
        target += (index // stride + shift // stride) % side * stride
    return target


def route(payload, shift, side):
    count = side**3

    def along(offset):
        pairs = [(i, shifted_target(i, offset, side)) for i in range(count)]
        return lambda block: lax.ppermute(block, "ka", pairs)

    middle = shift // side % side
    outer = shift // (side * side) * side + shift % side
    ends = [i // side * side * side + i % side for i in range(1, side * side)]
    payload = lax.switch(middle, [lambda block: block] + [along(i * side) for i in range(1, side)], payload)
    return lax.switch(outer, [lambda block: block] + [along(i) for i in ends], payload)


def per_device(
    val_wave, cond_wave, val_energy, cond_energy, frequency, kpoint_map, umklapp, gvector_index
):
    slab_count = lax.axis_size("slab")
    kpoint_count = lax.axis_size("ka")
    side = max((candidate for candidate in range(1, 9) if candidate**3 <= kpoint_count))
    shift = kpoint_map[0]
    planes, extent_y, extent_z = val_wave.shape[3:]
    fields = val_wave.shape[0] * val_wave.shape[2] * planes
    levels = jnp.pad(val_energy, ((0, extent_y - 1), (0, extent_z - val_energy.shape[1])))
    packed = jnp.concatenate([val_wave.reshape(fields, extent_y, extent_z), levels[None]], 0)
    packed = route(packed, shift, side)
    points = planes * slab_count * extent_y * extent_z
    norm = 1.0 / (2.0 * math.sqrt(points))
    freq_count = frequency.shape[0]
    total_g = gvector_index.shape[0]
    row_g = total_g // kpoint_count
    product = kernel_call(
        kpoint_map, frequency, cond_energy, packed, cond_wave[:, 0], gvector_index[None], norm,
        slab_count, kpoint_count,
    )
    return product.reshape(freq_count, 2, row_g, total_g // slab_count)


def solution(mesh):
    return jax.shard_map(
        per_device,
        mesh=mesh,
        in_specs=(
            P(None, "ka", None, "slab", None, None),
            P(None, "ka", None, "slab", None, None),
            P("ka", None),
            P("ka", None),
            P(),
            P(),
            P(),
            P(),
        ),
        out_specs=P(None, None, "ka", "slab"),
        check_vma=False,
    )
```

```python
import functools
import math

import jax
import jax.numpy as jnp
import numpy as np
from jax import lax
from jax.experimental import pallas as pl
from jax.experimental.pallas import tpu as pltpu
from jax.sharding import PartitionSpec as P

HIGH = lax.Precision.HIGHEST
MESH = pl.DeviceIdType.MESH
f32, bf16 = jnp.float32, jnp.bfloat16
TILE = 768
SIDE = 4
CUT = 384
EXTRA = 128
WIDE = 768
FIRST = 0
ORDER = (
    0, 1, 5, 2, 6, 4, 3, 8, 7, 9, 85, 86, 90, 87, 10, 14, 89, 11, 44, 47, 50, 17, 91, 93, 88, 92,
    94, 49, 15, 16, 48, 18, 19, 52, 51, 30, 13, 23, 12, 63, 46, 20, 53, 21, 45, 56, 95, 96, 99, 129,
    132, 102, 135, 54, 31, 32, 33, 25, 26, 24, 65, 66, 64, 55, 22, 37, 58, 101, 100, 104, 103, 134,
    137, 70, 57, 59, 98, 115, 133, 136, 97, 108, 34, 27, 131, 148, 130, 141, 35, 68, 28, 38, 39, 40,
    67, 105, 77, 122, 106, 71, 73, 61, 60, 155, 138, 117, 72, 116, 118, 139, 110, 109, 36, 111, 78,
    149, 150, 142, 29, 124, 151, 41, 144, 69, 143, 123, 125, 107, 157, 75, 62, 140, 42, 74, 156,
    158, 119, 120, 112, 81, 113, 152, 153, 43, 79, 145, 146, 126, 127, 162, 76, 82, 121, 159, 80,
    154, 160, 114, 147, 163, 128, 83, 161, 166, 164, 168, 84, 167, 165, 169,
)


def y_table(bands, extent):
    index = np.arange(extent)
    angle = 2 * np.pi * (np.outer(index, index) % extent) / extent
    eye = np.eye(bands)
    size = bands * extent
    cos = np.einsum("ky,cd->kcdy", np.cos(angle), eye).reshape(size, size)
    sin = np.einsum("ky,cd->kcdy", np.sin(angle), eye).reshape(size, size)
    return np.block([[cos, sin], [-sin, cos]]).astype(np.float32)


def z_table(extent):
    index = np.arange(extent)
    angle = 2 * np.pi * (np.outer(index, index) % extent) / extent
    cos, sin = np.cos(angle), np.sin(angle)
    return np.block([[cos, -sin], [sin, cos]]).astype(np.float32)


def x_phases(extent, planes, norm):
    angle = 2 * np.pi * (np.outer(np.arange(planes), np.arange(extent)) % extent) / extent
    return np.cos(angle) * norm, np.sin(angle) * norm


def split_rows(value):
    high = value.astype(bf16)
    return high, (value - high.astype(f32)).astype(bf16)


def thrice(table, axis):
    high, low = jnp.split(table, 2, axis)
    return jnp.concatenate([high, high, low], axis)


def split_table(table, axis):
    high = table.astype(jnp.bfloat16)
    low = (table - high.astype(np.float32)).astype(jnp.bfloat16)
    return jnp.asarray(np.concatenate([high, low], axis))


def kernel(
    kpoints, row_g, norm, packed, shift_in, freq_in, cond_e_in, gvec_in, cond_in, ytab_in, ztab_in, out,
    g00, g01, g10, g11, part, r1, s2, r2, spec, phase, wtile, rt, left, sel, wsel,
    shift, freq, cond_e, cond, gvec, ytab, ztab, counter, loads,
    send, recv, rsend, rrecv,
):
    inputs = (shift_in, freq_in, cond_e_in, gvec_in, cond_in, ytab_in, ztab_in)
    held_here = (shift, freq, cond_e, gvec, cond, ytab, ztab)
    fetches = [
        pltpu.make_async_copy(there, here, loads.at[i])
        for i, (there, here) in enumerate(zip(inputs, held_here))
    ]
    for fetch in fetches:
        fetch.start()
    ka = lax.axis_index("ka")
    slab = lax.axis_index("slab")
    zlo, core = slab // 2, slab % 2
    block_g = part.shape[3]
    half_g = block_g // 2
    freqs = freq.shape[0]
    coords = (ka // (SIDE * SIDE), ka // SIDE % SIDE, ka % SIDE)
    xi, hi, yi = coords
    bands, planes, ny, nz = cond.shape[1:]
    nv = 2
    nx = planes * 4
    rows = bands * ny
    height = planes * 2 * bands
    fields = nv * 2 * planes
    bufs = ((g00, g01), (g10, g11))

    def neighbour(axis, move):
        if axis == "x":
            return ((xi + move) % SIDE * 16 + hi * 4 + yi, slab)
        if axis == "h":
            return (xi * 16 + (hi + move) % SIDE * 4 + yi, slab)
        return (xi * 16 + hi * 4 + (yi + move) % SIDE, slab)

    peers = [(ka, (slab + d) % 4) for d in range(1, 4)]
    partner = (ka, zlo * 2 + 1 - core)
    across = (ka, (1 - zlo) * 2 + core)

    barrier = pltpu.get_barrier_semaphore()
    friends = [neighbour(axis, move) for axis in "xhy" for move in (1, 3)] + peers
    for friend in friends:
        pl.semaphore_signal(barrier, inc=1, device_id=friend, device_id_type=MESH)

    copies, waited = {}, set()

    def start(name, src, dst, device):
        k = len(copies)
        c = pltpu.make_async_remote_copy(
            src_ref=src, dst_ref=dst, send_sem=send.at[k], recv_sem=recv.at[k],
            device_id=device, device_id_type=MESH,
        )
        copies[name] = c
        c.start()

    def need(*names):
        for name in names:
            if name not in waited:
                waited.add(name)
                copies[name].wait_recv()

    for fetch in fetches:
        fetch.wait()

    q = shift[0]
    folds = [
        (coords[d] < q // SIDE ** (2 - d) % SIDE).astype(jnp.int32) for d in range(3)
    ]
    targets = [
        (1 - zlo) * 2 + 1 - core,
        (1 - zlo) * 2 + core,
        zlo * 2 + 1 - core,
        zlo * 2 + core,
    ]

    owner = ka * row_g // block_g
    at = ka * row_g - owner * block_g
    side_q = at // half_g
    line = lax.broadcasted_iota(jnp.int32, sel.shape, 0)
    lane = lax.broadcasted_iota(jnp.int32, sel.shape, 1)
    sel[...] = (lane == line + at - side_q * half_g).astype(f32).astype(bf16)
    for v in range(nv):
        line = lax.broadcasted_iota(jnp.int32, wsel.shape[1:], 0)
        lane = lax.broadcasted_iota(jnp.int32, wsel.shape[1:], 1)
        wsel[v] = ((lane == line + 3 * freqs * v) & (line < 3 * freqs)).astype(f32).astype(bf16)

    def weights():
        shape = (2 * bands, EXTRA)
        lane = lax.broadcasted_iota(jnp.int32, shape, 1)
        row = lax.broadcasted_iota(jnp.int32, shape, 0)
        level = jnp.zeros(shape, f32)
        for c in range(bands):
            level = jnp.where((row == c) | (row == bands + c), cond_e[0, c], level)
        omega = jnp.ones(shape, f32)
        value = jnp.zeros(shape, f32)
        for v in range(nv):
            for w in range(freqs):
                first = 3 * (v * freqs + w)
                omega = jnp.where((lane >= first) & (lane < first + 3), freq[w], omega)
        for v in range(nv):
            gap = packed[fields, v * ny // nv : v * ny // nv + 1, 0:1] - level
            weight = 2.0 * gap / (gap * gap + omega * omega) / kpoints
            high = weight.astype(bf16).astype(f32)
            mid = (weight - high).astype(bf16).astype(f32)
            low = weight - high - mid
            piece = lane % 3
            pieces = jnp.where(piece == 0, high, jnp.where(piece == 1, mid, low))
            first = 3 * v * freqs
            value = jnp.where((lane >= first) & (lane < first + 3 * freqs), pieces, value)
        wtile[...] = value.astype(bf16)

    def spectrum(v):
        columns = []
        for x in range(planes):
            vr = packed[v * planes + x][None]
            vi = packed[(nv + v) * planes + x][None]
            cr, ci = cond[0, :, x], cond[1, :, x]
            re = (vr * cr + vi * ci).reshape(rows, nz)
            im = (vr * ci - vi * cr).reshape(rows, nz)
            columns.append(jnp.concatenate([re, im], 0))
        high, low = split_rows(jnp.concatenate(columns, 1))
        t = jnp.dot(thrice(ytab[...], 1), jnp.concatenate([high, low, high], 0), preferred_element_type=f32)
        t = [
            jnp.concatenate([t[:rows, x * nz : (x + 1) * nz], t[rows:, x * nz : (x + 1) * nz]], 1)
            for x in range(planes)
        ]
        high, low = split_rows(jnp.concatenate(t, 0))
        f = jnp.dot(jnp.concatenate([high, low, high], 1), thrice(ztab[...], 0), preferred_element_type=f32)
        for x in range(planes):
            fx = f[x * rows : (x + 1) * rows]
            both = [fx[:, :nz].reshape(ny, bands, nz), fx[:, nz:].reshape(ny, bands, nz)]
            both = jnp.concatenate(both, 1).reshape(ny // 2, 2, 2 * bands, nz)
            for odd in range(2):
                high, low = split_rows(both[:, odd])
                here = slice(2 * bands * x, 2 * bands * (x + 1))
                spec[:, here, odd * nz : (odd + 1) * nz] = high
                spec[:, here, (2 + odd) * nz : (3 + odd) * nz] = low

    def columns_of(v, j, tile=None):
        def step(i, _):
            cols = pl.ds(pl.multiple_of(targets[j] * block_g + i * TILE, TILE), TILE)
            local = pl.ds(pl.multiple_of(i * TILE, TILE), TILE)
            g = gvec[:, cols]
            gz = (g - folds[2] + nz) & (nz - 1)
            gy = ((g >> 7) - folds[1] + ny) & (ny - 1)
            if v == 0:
                gx = (g >> 11) - folds[0]
                gx = jnp.where(gx < 0, gx + nx, gx)
                turn = (slab * gx) & 3
                flip = (turn & 1) == 1
                sign = jnp.where(turn >= 2, -1.0, 1.0)
                cos_of, sin_of = x_phases(nx, planes, norm)
                cosines, sines = [], []
                for x in range(planes):
                    c, s = jnp.full((1, TILE), norm, f32), jnp.zeros((1, TILE), f32)
                    for m in range(1, nx if x else 1):
                        c = jnp.where(gx == m, float(cos_of[x, m]), c)
                        s = jnp.where(gx == m, float(sin_of[x, m]), s)
                    cosines.append(sign * jnp.where(flip, -s, c))
                    sines.append(sign * jnp.where(flip, c, s))
                for x in range(planes):
                    phase[x : x + 1, cols] = cosines[x]
                    phase[planes + x : planes + x + 1, cols] = sines[x]
            else:
                cosines = [phase[x : x + 1, cols] for x in range(planes)]
                sines = [phase[planes + x : planes + x + 1, cols] for x in range(planes)]
            code = gz + (gy & 1) * nz
            same = counter[...] == jnp.broadcast_to(code.astype(f32).astype(bf16), counter.shape)
            hot = jnp.where(same, jnp.ones(counter.shape, bf16), jnp.zeros(counter.shape, bf16))
            hot = jnp.concatenate([hot, hot], 0)
            table = spec[...].reshape(ny // 2 * height, 4 * nz)
            picked = jnp.dot(table, hot, preferred_element_type=f32)
            which = jnp.broadcast_to(gy >> 1, (height, TILE))
            acc = picked[:height]
            for k in range(1, ny // 2):
                acc = jnp.where(which == k, picked[k * height : (k + 1) * height], acc)
            re, im = 0.0, 0.0
            for x in range(planes):
                a = x * 2 * bands
                sre, sim = acc[a : a + bands], acc[a + bands : a + 2 * bands]
                re = re + (sre * cosines[x] + sim * sines[x])
                im = im + (sim * cosines[x] - sre * sines[x])
            part[v, j, :, local] = jnp.concatenate([re, im], 0)
            return 0

        if tile is not None:
            step(tile, 0)
        else:
            lax.fori_loop(0, block_g // TILE, step, 0)

    actions = {}

    def add(name, call):
        actions[name] = call

    def tile_cols(i):
        return pl.ds(i * TILE, TILE)

    def compute(v, j, i):
        def call():
            columns_of(v, j, i)
            if (v, j, i) == (0, 0, 0):
                pl.semaphore_wait(barrier, len(friends))
            if j == 0:
                here = part.at[v, 0, :, tile_cols(i)]
                start(f"ra{v}{i}", here, r1.at[v, 0, :, tile_cols(i)], partner)
            if j == 2 and i == block_g // TILE - 1:
                start(f"rb{v}", part.at[v, 2], r1.at[v, 1], partner)

        return call

    def across_sum(v, i):
        def call():
            need(f"ra{v}{i}")
            cols = tile_cols(i)
            s2[v, :, cols] = part[v, 1, :, cols] + r1[v, 0, :, cols]
            start(f"r2{v}{i}", s2.at[v, :, cols], r2.at[v, :, cols], across)

        return call

    def finish_block(v):
        def call():
            need(f"rb{v}", *[f"r2{v}{i}" for i in range(block_g // TILE)])
            total = (part[v, 3] + r1[v, 1] + r2[v]).astype(bf16)
            bufs[v][0][0, 0, 0] = total[:, :half_g]
            if v == 0:
                bufs[v][1][0, 0, 0, :, :half_g] = total[:, half_g:]
                bufs[v][1][0, 0, 0, :, half_g:] = wtile[...]
            else:
                bufs[v][1][0, 0, 0] = total[:, half_g:]

        return call

    def ring(one, two, names, axis, slots, low, high):
        def begin():
            start(one + "p", slots(0), slots(1), neighbour(axis, 1))
            start(one + "m", slots(0), slots(2), neighbour(axis, 3))

        def forward():
            need(one + "p")
            start(two + "p", low(slots(1)), low(slots(3)), neighbour(axis, 1))

        def back():
            need(one + "m")
            start(two + "m", high(slots(2)), high(slots(3)), neighbour(axis, 3))

        for name, call in zip(names, (begin, forward, back)):
            add(name, call)

    def after(events, name):
        inner_call = actions[name]

        def call():
            need(*events)
            inner_call()

        actions[name] = call

    def low_lanes(ref):
        return ref.at[:, pl.ds(0, CUT)]

    def high_lanes(ref):
        return ref.at[:, pl.ds(CUT, ref.shape[1] - CUT)]

    def low_blocks(ref):
        return ref.at[pl.ds(0, 2)]

    def high_blocks(ref):
        return ref.at[pl.ds(2, 2)]

    def units_of(h):
        if h == 0:
            return {"0": (0, 1), "1": (1, 1), "2": (2, 1), "3": (3, 1)}
        return {"a": (0, 2), "b": (2, 2)}

    def fine(v, side, h, axis):
        g = bufs[v][side]
        k = f"{v}{side}{h}"
        ready = ((), (f"I{k}1p",), (f"I{k}1m",), (f"I{k}2p", f"I{k}2m"))
        units = units_of(h)

        def begin(unit, first, count):
            def call():
                for i in range(first, first + count):
                    need(*ready[i])
                blocks = pl.ds(first, count)
                for way, slot, move in (("p", 1, 1), ("m", 2, 3)):
                    start(
                        f"O{k}{way}{unit}", g.at[h, 0, blocks], g.at[h, slot, blocks],
                        neighbour(axis, move),
                    )

            return call

        def turn(way, first, slot, move):
            def call():
                for unit, (at, count) in units.items():
                    if first <= at < first + 2:
                        need(f"O{k}{way}{unit}")
                blocks = pl.ds(first, 2)
                start(f"O{k}2{way}", g.at[h, slot, blocks], g.at[h, 3, blocks], neighbour(axis, move))

            return call

        for unit, (first, count) in units.items():
            add(f"Os{unit}{k}", begin(unit, first, count))
        add(f"Otp{k}", turn("p", 0, 1, 1))
        add(f"Otm{k}", turn("m", 2, 2, 3))

    row_copies = {}

    def natural(v, side, h, cols):
        g = bufs[v][side]
        if side:
            return g[h, :, :, :, cols].reshape(SIDE * SIDE * 2 * bands, -1)
        return jnp.concatenate([g[h, y, x, :, cols] for x in range(SIDE) for y in range(SIDE)], 0)

    transposed = (((1,), (1,)), ((), ()))

    def ship_rows(v, h):
        chunk = v * SIDE + h

        def call():
            for side in range(2):
                for way in "pm":
                    need(f"O{v}{side}{h}2{way}", *[f"O{v}{side}{h}{way}{u}" for u in units_of(h)])
                    need(f"O01{h}2{way}", *[f"O01{h}{way}{u}" for u in units_of(h)])
            held = [
                pltpu.make_async_remote_copy(
                    src_ref=rt.at[chunk], dst_ref=rt.at[chunk], send_sem=rsend.at[chunk, d],
                    recv_sem=rrecv.at[chunk], device_id=peers[d], device_id_type=MESH,
                )
                for d in range(3)
            ]
            row_copies[chunk] = held

            @pl.when(slab == owner)
            def _():
                tiles = natural(0, 1, h, pl.ds(half_g, EXTRA))
                w = lax.dot_general(wsel[v], tiles, transposed, preferred_element_type=f32)
                rt[chunk, row_g:] = w.astype(bf16)
                for side in range(2):

                    @pl.when(side_q == side)
                    def _():
                        block = natural(v, side, h, pl.ds(0, half_g))
                        picked = lax.dot_general(sel[...], block, transposed, preferred_element_type=f32)
                        rt[chunk, :row_g] = picked.astype(bf16)

                for c in held:
                    c.start()

        return call

    def multiply(v, h):
        chunk = v * SIDE + h

        def call():
            @pl.when(slab != owner)
            def _():
                row_copies[chunk][0].wait_recv()

            both = rt[chunk].astype(f32)
            base = both[:row_g]
            spot = lax.broadcasted_iota(jnp.int32, base.shape, 1)
            swapped = jnp.where(spot % 16 < 8, pltpu.roll(base, 248, 1), -pltpu.roll(base, 8, 1))
            for w in range(freqs):
                k = row_g + 3 * w
                scale = both[k : k + 1] + both[k + 1 : k + 2] + both[k + 2 : k + 3]
                left[2 * w * row_g : (2 * w + 1) * row_g] = (base * scale).astype(bf16)
                left[(2 * w + 1) * row_g : (2 * w + 2) * row_g] = (swapped * scale).astype(bf16)
            for side in range(2):

                def column(i, _, side=side):
                    cols = pl.ds(pl.multiple_of(i * WIDE, WIDE), WIDE)
                    there = pl.ds(pl.multiple_of(side * half_g + i * WIDE, WIDE), WIDE)
                    product = jnp.dot(left[...], natural(v, side, h, cols), preferred_element_type=f32)
                    if chunk == FIRST:
                        out[:, there] = product
                    else:
                        out[:, there] += product
                    return 0

                lax.fori_loop(0, half_g // WIDE, column, 0)

        return call

    for v in range(nv):
        add(f"S{v}", lambda v=v: spectrum(v))
        tiles = block_g // TILE
        for i in range(tiles):
            for j in range(3):
                add(f"T{v}{j}{i}", compute(v, j, i))
            add(f"rs{v}{i}", across_sum(v, i))
        add(f"C{v}3", lambda v=v: columns_of(v, 3))
        add(f"fin_{v}", finish_block(v))
        for side in range(2):
            g = bufs[v][side]
            k = f"{v}{side}"
            inner, outer = ("x", "y") if side == 0 else ("y", "x")
            ring(f"H{k}1", f"H{k}2", (f"Hs{k}", f"Htp{k}", f"Htm{k}"), "h",
                 lambda j, g=g: g.at[j, 0, 0], low_lanes, high_lanes)
            for h in range(SIDE):
                ring(f"I{k}{h}1", f"I{k}{h}2", (f"Is{k}{h}", f"Itp{k}{h}", f"Itm{k}{h}"), inner,
                     lambda j, g=g, h=h: g.at[h, 0, j], low_lanes, high_lanes)
                fine(v, side, h, outer)
                before = ((), (f"H{k}1p",), (f"H{k}1m",), (f"H{k}2p", f"H{k}2m"))[h]
                after(before, f"Is{k}{h}")
        for h in range(SIDE):
            add(f"R{v}{h}", ship_rows(v, h))
            add(f"M{v}{h}", multiply(v, h))

    counter[...] = lax.broadcasted_iota(jnp.int32, counter.shape, 0).astype(f32).astype(bf16)
    weights()
    steps = list(actions.values())
    assert sorted(ORDER) == list(range(len(steps)))
    for at in ORDER:
        steps[at]()

    for c in copies.values():
        c.wait_send()

    @pl.when(slab == owner)
    def _():
        for held in row_copies.values():
            for c in held:
                c.wait_send()


def kernel_call(shift, freq, cond_e, packed, cond, gvec, norm, slabs, kpoints):
    bands, planes, ny, nz = cond.shape[1:]
    ytab, ztab = split_table(y_table(bands, ny), 1), split_table(z_table(nz), 0)
    fetched = (shift, freq, cond_e, gvec, cond, ytab, ztab)
    total = gvec.shape[1]
    block_g, row_g, freqs = total // slabs, total // kpoints, freq.shape[0]
    half = 2 * bands
    tall = (row_g + 3 * freqs + 15) // 16 * 16
    vm = pl.BlockSpec(memory_space=pltpu.VMEM)
    far = pl.BlockSpec(memory_space=pltpu.HBM)
    count = 2 * (3 + 1 + 3) + 4 * (4 + 16 + 10 + 3 * 6)
    return pl.pallas_call(
        functools.partial(kernel, float(kpoints), row_g, norm),
        out_shape=jax.ShapeDtypeStruct((freqs * 2 * row_g, block_g), f32),
        in_specs=[vm] + [far] * 7,
        out_specs=vm,
        scratch_shapes=[
            pltpu.VMEM((4, 4, 4, half, block_g // 2), bf16),
            pltpu.VMEM((4, 4, 4, half, block_g // 2 + EXTRA), bf16),
            pltpu.VMEM((4, 4, 4, half, block_g // 2), bf16),
            pltpu.VMEM((4, 4, 4, half, block_g // 2), bf16),
            pltpu.VMEM((2, 4, half, block_g), f32),
            pltpu.VMEM((2, 2, half, block_g), f32),
            pltpu.VMEM((2, half, block_g), f32),
            pltpu.VMEM((2, half, block_g), f32),
            pltpu.VMEM((ny // 2, planes * half, 4 * nz), bf16),
            pltpu.VMEM((8, total), f32),
            pltpu.VMEM((half, EXTRA), bf16),
            pltpu.VMEM((8, tall, 256), bf16),
            pltpu.VMEM((freqs * 2 * row_g, 256), bf16),
            pltpu.VMEM((row_g, block_g // 2), bf16),
            pltpu.VMEM((2, tall - row_g, EXTRA), bf16),
            pltpu.SMEM(shift.shape, jnp.int32),
            pltpu.SMEM(freq.shape, f32),
            pltpu.SMEM(cond_e.shape, f32),
            pltpu.VMEM(cond.shape, f32),
            pltpu.VMEM(gvec.shape, jnp.int32),
            pltpu.VMEM(ytab.shape, bf16),
            pltpu.VMEM(ztab.shape, bf16),
            pltpu.VMEM((2 * nz, TILE), bf16),
            pltpu.SemaphoreType.DMA((7,)),
            pltpu.SemaphoreType.DMA((count,)),
            pltpu.SemaphoreType.DMA((count,)),
            pltpu.SemaphoreType.DMA((8, 3)),
            pltpu.SemaphoreType.DMA((8,)),
        ],
        compiler_params=pltpu.CompilerParams(
            collective_id=0, has_side_effects=True, vmem_limit_bytes=46_000_000
        ),
        cost_estimate=pl.CostEstimate(flops=10**10, bytes_accessed=10**7, transcendentals=0),
        name="response",
    )(
        packed, *[pltpu.with_memory_space_constraint(a, pltpu.HBM) for a in fetched],
    )


def shifted_target(index, shift, side):
    target = 0
    for stride in (side * side, side, 1):
        target += (index // stride + shift // stride) % side * stride
    return target


def route(payload, shift, side):
    count = side**3

    def along(offset):
        pairs = [(i, shifted_target(i, offset, side)) for i in range(count)]
        return lambda block: lax.ppermute(block, "ka", pairs)

    middle = shift // side % side
    outer = shift // (side * side) * side + shift % side
    ends = [i // side * side * side + i % side for i in range(1, side * side)]
    payload = lax.switch(middle, [lambda block: block] + [along(i * side) for i in range(1, side)], payload)
    return lax.switch(outer, [lambda block: block] + [along(i) for i in ends], payload)


def per_device(
    val_wave, cond_wave, val_energy, cond_energy, frequency, kpoint_map, umklapp, gvector_index
):
    slab_count = lax.axis_size("slab")
    kpoint_count = lax.axis_size("ka")
    side = max((candidate for candidate in range(1, 9) if candidate**3 <= kpoint_count))
    shift = kpoint_map[0]
    planes, extent_y, extent_z = val_wave.shape[3:]
    fields = val_wave.shape[0] * val_wave.shape[2] * planes
    levels = jnp.broadcast_to(val_energy.reshape(1, -1, 1, 1), (1, val_energy.shape[1], extent_y // 2, extent_z))
    levels = levels.reshape(1, extent_y, extent_z)
    packed = jnp.concatenate([val_wave.reshape(fields, extent_y, extent_z), levels], 0)
    packed = route(packed, shift, side)
    points = planes * slab_count * extent_y * extent_z
    norm = 1.0 / (2.0 * math.sqrt(points))
    freq_count = frequency.shape[0]
    total_g = gvector_index.shape[0]
    row_g = total_g // kpoint_count
    product = kernel_call(
        kpoint_map, frequency, cond_energy, packed, cond_wave[:, 0], gvector_index[None], norm,
        slab_count, kpoint_count,
    )
    return product.reshape(freq_count, 2, row_g, total_g // slab_count)


def solution(mesh):
    return jax.shard_map(
        per_device,
        mesh=mesh,
        in_specs=(
            P(None, "ka", None, "slab", None, None),
            P(None, "ka", None, "slab", None, None),
            P("ka", None),
            P("ka", None),
            P(),
            P(),
            P(),
            P(),
        ),
        out_specs=P(None, None, "ka", "slab"),
        check_vma=False,
    )
```
